256 devices in a mesh: dp: 64 (over z, x, core), outer: 4 (over y).
Axes of the slice: x: 4, y: 4, z: 8, core: 2. Of those that a mesh axis runs over, the one named last changes fastest.
Arguments:
- partials: bfloat16 [4, 64, 2, 128, 8192], P('outer', 'dp'), may hold values from -3500 to 3500, as said below
- master: float32 [2, 128, 8192], P(None, 'dp'), may hold values from -6 to 6
- m_codes: bfloat16 [2, 128, 8192], P(None, 'dp'), may hold values from -1 to 1
- v_codes: bfloat16 [2, 128, 8192], P(None, 'dp'), may hold values from 0.049804688 to 1
- m_scales: float32 [2, 128, 4], P(None, 'dp'), may hold values from 0.0001 to 0.001
- v_scales: float32 [2, 128, 4], P(None, 'dp'), may hold values from 1e-08 to 1e-07
Outputs:
- new_master: float32 [2, 128, 8192], P(None, 'dp')
- new_m_codes: bfloat16 [2, 128, 8192], P(None, 'dp')
- new_v_codes: bfloat16 [2, 128, 8192], P(None, 'dp')
- new_m_scales: float32 [2, 128, 4], P(None, 'dp')
- new_v_scales: float32 [2, 128, 4], P(None, 'dp')
- weights: bfloat16 [2, 128, 8192], replicated
The draws below stay inside these ranges and needn't reach their ends.
Inputs may be any that keep to these rules, and one draw needn't show every extreme that they name: Gradient partials of real values; entries vary from row to row and column to column.
All inputs are finite; a program needn't handle non-finite values. Where the reference program divides by a largest or mean magnitude, that divisor is 1e-20 or more.
Results may differ from the reference program's by a relative error of at most 0.0004.
Values may be sent and summed in bfloat16 or wider, within the bound.
A program may use at most 64 MiB of HBM per device.

```python
import math
import jax
import jax.numpy as jnp
from jax import lax

D = 8192
BLOCK = 2048
STEP = 10
V = 128
REPLICAS = 64
GROUPS = 4


def draw_partials(key, part):
    keys = jax.random.split(jax.random.fold_in(key, 17), 3)
    shape_full = (GROUPS, REPLICAS, 2, V, D)
    ramp = 1.0 + 2.0 * jnp.arange(V, dtype=jnp.float32) / max(V - 1, 1)
    row_scale = jnp.exp(jax.random.uniform(keys[1], (2, V, 1), jnp.float32) * math.log(10.0)) * ramp[None, :, None]
    col_scale = jnp.exp(jax.random.uniform(keys[2], (2, 1, D), jnp.float32) * math.log(10.0))
    base = jnp.clip(jax.random.normal(keys[0], shape_full, jnp.float32), -6.0, 6.0)
    return (base * row_scale[None, None] * col_scale[None, None]).astype(jnp.bfloat16)


def shard_levels(rng, dims, shards, low, top_value):
    factor_of, own = 1.0, jax.random.fold_in(rng, 6)
    for position, shards_of in shards:
        heights = jnp.exp(jax.random.uniform(jax.random.fold_in(own, position), (shards_of,), jnp.float32, low / len(shards), top_value / len(shards)))
        factor_of = factor_of * jnp.repeat(heights, dims[position] // shards_of).reshape([-1 if axis == position else 1 for axis in range(len(dims))])
    return factor_of


def centred(own_key, dims, scale, limit, cuts=(), kind=jnp.bfloat16):
    loudness = shard_levels(own_key, dims, cuts, -0.22, 0.18) if cuts else 1.0
    result = jax.random.normal(own_key, dims, jnp.float32) * scale * loudness
    return jnp.minimum(jnp.maximum(result, -limit), limit).astype(kind)


def setup_inputs(seed: int = 0) -> dict:
    streams_of = jax.random.split(jax.random.key(seed), 7)
    return {
        "partials": draw_partials(jax.random.fold_in(streams_of[6], 71), 0),
        "master": centred(streams_of[1], (2, V, D), 1.0, 6.0, ((1, 64),), jnp.float32),
        "m_codes": jnp.clip(jax.random.uniform(streams_of[2], (2, V, D), jnp.float32, -1.0, 1.0) * shard_levels(streams_of[2], (2, V, D), ((1, 64),), -0.4, 0.0), -1.0, 1.0).astype(jnp.bfloat16),
        "v_codes": jnp.clip(0.049804688 + 0.9501953 * jax.random.uniform(streams_of[3], (2, V, D), jnp.float32) ** shard_levels(streams_of[3], (2, V, D), ((1, 64),), -0.2, 0.2), 0.049804688, 1.0).astype(jnp.bfloat16),
        "m_scales": jnp.clip(jnp.exp(math.log(0.001) - 2.3025852 * jax.random.uniform(streams_of[4], (2, V, D // BLOCK), jnp.float32) ** shard_levels(streams_of[4], (2, V, D // BLOCK), ((1, 64),), -0.2, 0.2)), 0.0001, 0.001),
        "v_scales": jnp.clip(jnp.exp(math.log(1.0000000116860974e-07) - 2.3025851 * jax.random.uniform(streams_of[5], (2, V, D // BLOCK), jnp.float32) ** shard_levels(streams_of[5], (2, V, D // BLOCK), ((1, 64),), -0.2, 0.2)), 9.99999993922529e-09, 1.0000000116860974e-07),
    }


def adam_blocks(gradient, master, m_codes, v_codes, m_scales, v_scales, clip_factor):
    count = gradient.shape[0]
    rows = gradient.shape[1]
    blocks = gradient.shape[2] // BLOCK
    shape_four = (count, rows, blocks, BLOCK)
    moment = m_codes.astype(jnp.float32).reshape(shape_four) * m_scales[..., None]
    second = v_codes.astype(jnp.float32).reshape(shape_four) * v_scales[..., None]
    scaled = clip_factor * gradient.reshape(shape_four)
    moment = 0.9 * moment + 0.1 * scaled
    second = 0.95 * second + 0.05 * scaled * scaled
    update = moment / (1.0 - 0.9 ** STEP) / (jnp.sqrt(second / (1.0 - 0.95 ** STEP)) + 1e-08)
    fresh = master - 0.01 * update.reshape(master.shape)
    m_top = lax.optimization_barrier(jnp.max(jnp.abs(moment), axis=3)) + 1e-20
    v_top = lax.optimization_barrier(jnp.max(jnp.abs(second), axis=3)) + 1e-20
    m_next = (moment / m_top[..., None]).astype(jnp.bfloat16).reshape(master.shape)
    v_next = (second / v_top[..., None]).astype(jnp.bfloat16).reshape(master.shape)
    return (fresh, m_next, v_next, m_top, v_top, fresh.astype(jnp.bfloat16))

def reference(partials, master, m_codes, v_codes, m_scales, v_scales):

    def add_group(total, group):
        return (total + lax.optimization_barrier(jnp.sum(group.astype(jnp.float32), axis=0)), None)
    start_sum = jnp.zeros(partials.shape[2:], jnp.float32)
    gradient, _ = lax.scan(add_group, start_sum, partials)
    norm_value = jnp.sqrt(jnp.sum(gradient * gradient))
    clip_factor = 1.0 / jnp.maximum(norm_value, 1.0)
    return adam_blocks(gradient, master, m_codes, v_codes, m_scales, v_scales, clip_factor)
```

```python
import functools

import jax
import jax.numpy as jnp
from jax import lax
from jax.experimental import pallas as pl
from jax.experimental.pallas import tpu as pltpu
from jax.sharding import Mesh
from jax.sharding import PartitionSpec as P

BLOCK = 2048
STEP = 10
MESH = pl.DeviceIdType.MESH
F32 = jnp.float32
BF16 = jnp.bfloat16

V = 128
D = 8192
HALF = 4096
WIDE = 1024
SUB = 256
NX, NY, NZ, NC = 4, 4, 8, 2
TILE = 16
SEMS = 256


def mod(a, n):
    return lax.rem(a + n, n)


def col(value, step):
    return pl.multiple_of(value, step)


def adam(moment, second, scaled, master):
    m2 = 0.9 * moment + 0.1 * scaled
    v2 = 0.95 * second + 0.05 * scaled * scaled
    update = m2 / (1.0 - 0.9**STEP) / (jnp.sqrt(v2 / (1.0 - 0.95**STEP)) + 1e-08)
    return m2, v2, master - 0.01 * update


def kernel(
    part_in, master_in, mc_in, vc_in, ms_in, vs_in,
    o_master, o_mc, o_vc, o_ms, o_vs, o_w,
    own, par, rcv1, snd, rcv2, s_buf, p2a, p2s, p2f, t_buf, z_buf, g_buf,
    nz, nxc, ny,
    e_master, e_mc, e_vc, e_s, sc_stage, mt, vt, wt,
    q_s, q_r, g_full,
    wbuf, l_master, l_mc, l_vc, l_ms, l_vs, r_master, r_mc, r_vc, r_ms, r_vs,
    ssem, rsem, lsem,
):
    x, y, z, c = (lax.axis_index(a) for a in ("x", "y", "z", "c"))
    other = 1 - c
    started, counts = [], [0, 0]

    def send(src, dst, **dev):
        k = counts[0]
        counts[0] += 1
        copy = pltpu.make_async_remote_copy(
            src_ref=src, dst_ref=dst, send_sem=ssem.at[k], recv_sem=rsem.at[k],
            device_id=dev, device_id_type=MESH,
        )
        copy.start()
        started.append(copy)
        return copy

    def local(src, dst):
        k = counts[1]
        counts[1] += 1
        copy = pltpu.make_async_copy(src, dst, lsem.at[k])
        copy.start()
        return copy

    axes = (("x", x, "y", y), ("y", y, "x", x))
    roles = [tuple(mod(i + d, 4) for d in (1, -1, 0, 2)) for _, i, _, _ in axes]
    roles2 = [tuple(mod(j + d, 4) for d in (1, -1, 0, 2)) for _, _, _, j in axes]
    own_k = 2 * x + c

    own_loads = [[None] * 3 for _ in range(2)]
    for role in range(3):
        for p in range(2):
            cols = pl.ds(col(p * HALF + roles[p][role] * WIDE, WIDE), WIDE)
            own_loads[p][role] = local(part_in.at[0, 0, c, :, cols], own.at[p, role])
    state_loads = [
        local(a, b)
        for a, b in (
            (ms_in, l_ms), (vs_in, l_vs), (master_in, l_master), (mc_in, l_mc), (vc_in, l_vc),
        )
    ]

    barrier = pltpu.get_barrier_semaphore()
    peers = []
    for d in range(1, 8):
        k = mod(own_k + d, 8)
        peers.append({"x": k // 2, "c": lax.rem(k, 2)})
    for d in range(1, 4):
        peers.append({"y": mod(y + d, 4)})
    for d in (1, -1):
        peers.append({"y": mod(y + d, 4), "c": other})
    for d in range(1, 8):
        peers.append({"z": mod(z + d, 8)})
    for dev in peers:
        pl.semaphore_signal(barrier, inc=1, device_id=dev, device_id_type=MESH)
    pl.semaphore_wait(barrier, len(peers))

    raw = [[[None] * 2 for _ in range(2)] for _ in range(2)]
    for q in range(2):
        m = lax.rem(c + q, 2)
        for p in range(2):
            axis = axes[p][0]
            for h in range(2):
                cols = pl.ds(col(p * HALF + roles[p][3] * WIDE + h * (WIDE // 2), WIDE // 2), WIDE // 2)
                raw[p][h][q] = send(
                    part_in.at[0, 0, m, :, cols], rcv1.at[p, h, q], **{axis: roles[p][h], "c": m}
                )
    pair = [[None] * 3 for _ in range(2)]
    for role in range(3):
        for p in range(2):
            cols = pl.ds(col(p * HALF + roles[p][role] * WIDE, WIDE), WIDE)
            pair[p][role] = send(part_in.at[0, 0, other, :, cols], par.at[p, role], c=other)

    ex = []
    tile_cols = [
        lambda kx: col(kx * WIDE + y * SUB, SUB),
        lambda kx: col(HALF + y * WIDE + kx * SUB, SUB),
    ]
    for d in range(8):
        k = mod(own_k + d, 8)
        kx, kc = k // 2, lax.rem(k, 2)
        for src, dst in ((master_in, e_master), (mc_in, e_mc), (vc_in, e_vc)):
            for p in range(2):
                s = src.at[kc, :, pl.ds(tile_cols[p](kx), SUB)]
                t = dst.at[own_k, p]
                if d == 0:
                    ex.append(local(s, t))
                else:
                    ex.append(send(s, t, x=kx, c=kc))

    plain = [[None] * 2 for _ in range(2)]
    for p in range(2):
        axis = axes[p][0]
        for side in range(2):
            own_loads[p][side].wait()
            pair[p][side].wait_recv()
            h = 1 - side
            lo = h * (WIDE // 2)

            @pl.loop(0, V // TILE)
            def _(t):
                rows = pl.ds(pl.multiple_of(t * TILE, TILE), TILE)
                cc = pl.ds(lo, WIDE // 2)
                snd[p, side, rows, cc] = own[p, side, rows, cc].astype(F32) + par[p, side, rows, cc].astype(F32)

            cc = pl.ds(lo, WIDE // 2)
            plain[p][side] = send(snd.at[p, side, :, cc], rcv2.at[p, side, :, cc], **{axis: roles[p][side]})

    for load in state_loads:
        load.wait()
    sc_stage[...] = jnp.zeros_like(sc_stage)
    for m in range(2):
        sc_stage[m, 0:2, 0:4] = l_ms[m]
        sc_stage[m, 2:4, 0:4] = l_vs[m]
    e_s[own_k] = sc_stage[c]
    for d in range(1, 8):
        k = mod(own_k + d, 8)
        kx, kc = k // 2, lax.rem(k, 2)
        ex.append(send(sc_stage.at[kc], e_s.at[own_k], x=kx, c=kc))

    relay = [[None] * 2 for _ in range(2)]
    for p in range(2):
        axis = axes[p][0]
        for side in range(2):
            h = side
            lo = h * (WIDE // 2)
            for q in range(2):
                raw[p][h][q].wait_recv()

            @pl.loop(0, V // TILE)
            def _(t):
                rows = pl.ds(pl.multiple_of(t * TILE, TILE), TILE)
                cc = pl.ds(lo, WIDE // 2)
                near = own[p, side, rows, cc].astype(F32) + par[p, side, rows, cc].astype(F32)
                far = rcv1[p, h, 0, rows, :].astype(F32) + rcv1[p, h, 1, rows, :].astype(F32)
                snd[p, side, rows, cc] = near + far

            cc = pl.ds(lo, WIDE // 2)
            relay[p][side] = send(snd.at[p, side, :, cc], rcv2.at[p, side, :, cc], **{axis: roles[p][side]})

    for copy in ex:
        copy.wait_recv()
    blocks = (x // 2, 2 + y // 2)
    for k in range(8):
        e = e_s[k]
        lane = lax.broadcasted_iota(jnp.int32, e.shape, 1)
        for p in range(2):
            scale = jnp.sum(jnp.where(lane == blocks[p], e, 0.0), axis=1, keepdims=True)
            rows = pl.ds(2 * k, 2)
            mt[p, rows, :] = e_mc[k, p].astype(F32) * scale[0:2]
            vt[p, rows, :] = e_vc[k, p].astype(F32) * scale[2:4]
            wt[p, rows, :] = e_master[k, p]

    half = SUB // 2
    for p in range(2):
        axis2 = axes[p][2]
        own_loads[p][2].wait()
        pair[p][2].wait_recv()
        for side in range(2):
            plain[p][side].wait_recv()
            relay[p][side].wait_recv()

        @pl.loop(0, V // TILE)
        def _(t):
            rows = pl.ds(pl.multiple_of(t * TILE, TILE), TILE)
            near = own[p, 2, rows, :].astype(F32) + par[p, 2, rows, :].astype(F32)
            s_buf[p, rows, :] = near + rcv2[p, 0, rows, :] + rcv2[p, 1, rows, :]

    first2 = [[None] * 2 for _ in range(2)]
    plain2 = [[None] * 2 for _ in range(2)]
    relay2 = [[None] * 2 for _ in range(2)]
    for p in range(2):
        axis2 = axes[p][2]
        r2 = roles2[p]
        for h in range(2):
            cols = pl.ds(col(r2[3] * SUB + h * half, half), half)
            first2[p][h] = send(s_buf.at[p, :, cols], p2a.at[p, h], **{axis2: r2[h]})
        for side in range(2):
            h = 1 - side
            cols = pl.ds(col(r2[side] * SUB + h * half, half), half)
            plain2[p][side] = send(s_buf.at[p, :, cols], p2f.at[p, side, h], **{axis2: r2[side]})
    for p in range(2):
        axis2 = axes[p][2]
        r2 = roles2[p]
        for side in range(2):
            h = side
            cols = pl.ds(col(r2[side] * SUB + h * half, half), half)
            first2[p][h].wait_recv()
            p2s[p, side] = s_buf[p, :, cols] + p2a[p, h]
            relay2[p][side] = send(p2s.at[p, side], p2f.at[p, side, h], **{axis2: r2[side]})
    zc = [[None] * 8 for _ in range(2)]
    for p in range(2):
        r2 = roles2[p]
        for side in range(2):
            plain2[p][side].wait_recv()
            relay2[p][side].wait_recv()
        for h in range(2):
            cols = pl.ds(col(r2[2] * SUB + h * half, half), half)
            t_buf[p, :, h * half:(h + 1) * half] = s_buf[p, :, cols] + p2f[p, 0, h] + p2f[p, 1, h]
        for d in (4, 3, 5, 2, 6, 1, 7):
            zd = mod(z + d, 8)
            rows = pl.ds(pl.multiple_of(zd * TILE, TILE), TILE)
            zc[p][d] = send(t_buf.at[p, rows, :], z_buf.at[p, d], z=zd)

    my_rows = pl.ds(pl.multiple_of(z * TILE, TILE), TILE)
    square = jnp.zeros((8, 128), F32)
    for p in range(2):
        g = t_buf[p, my_rows, :]
        for d in range(1, 8):
            zc[p][d].wait_recv()
            g = g + z_buf[p, d]
        g_buf[p] = g
        sq = g * g
        for i in range(2):
            for j in range(2):
                square = square + sq[8 * i:8 * i + 8, 128 * j:128 * j + 128]
    nz[z] = square
    n1 = [send(nz.at[z], nz.at[z], z=mod(z + d, 8)) for d in (4, 3, 5, 2, 6, 1, 7)]

    for p in range(2):
        for k in range(8):
            q_s[k, p] = g_buf[p, 2 * k:2 * k + 2, :]
    q1 = []
    for d in range(1, 8):
        k = mod(own_k + d, 8)
        q1.append(send(q_s.at[k], q_r.at[own_k], x=k // 2, c=lax.rem(k, 2)))
    q_r[own_k] = q_s[own_k]

    for copy in n1:
        copy.wait_recv()
    nxc[own_k] = functools.reduce(lambda a, b: a + b, [nz[k] for k in range(8)])
    n2 = []
    for d in range(1, 8):
        k = mod(own_k + d, 8)
        n2.append(send(nxc.at[own_k], nxc.at[own_k], x=k // 2, c=lax.rem(k, 2)))

    for copy in q1:
        copy.wait_recv()
    q2 = [send(q_r, g_full.at[y], y=mod(y + d, 4)) for d in range(1, 4)]
    g_full[y] = q_r[...]

    for copy in n2:
        copy.wait_recv()
    ny[y] = functools.reduce(lambda a, b: a + b, [nxc[k] for k in range(8)])
    n3 = [send(ny.at[y], ny.at[y], y=mod(y + d, 4)) for d in (2, 1, 3)]
    for copy in n3:
        copy.wait_recv()
    total = functools.reduce(lambda a, b: a + b, [ny[k] for k in range(4)])
    total = jnp.sum(jnp.sum(total, axis=1, keepdims=True), axis=0, keepdims=True)
    clip = 1.0 / jnp.maximum(jnp.sqrt(total), 1.0)

    block_of = lambda p, i, j: pl.ds(col(p * HALF + i * WIDE + j * SUB, SUB), SUB)
    for p in range(2):
        i1, i2 = axes[p][1], axes[p][3]
        _, _, fresh = adam(mt[p], vt[p], clip * g_buf[p], wt[p])
        wbuf[c, my_rows, block_of(p, i1, i2)] = fresh.astype(BF16)
    ag1 = [[], []]
    for d in (4, 3, 5, 2, 6, 1, 7):
        for p in range(2):
            ref = wbuf.at[c, my_rows, block_of(p, axes[p][1], axes[p][3])]
            ag1[p].append(send(ref, ref, z=mod(z + d, 8)))

    for copy in q2:
        copy.wait_recv()
    lane4 = lax.broadcasted_iota(jnp.int32, (2, 4), 1)
    for m in range(2):
        tops_m = jnp.zeros((2, 4), F32)
        tops_v = jnp.zeros((2, 4), F32)
        for b in range(4):
            cs = slice(b * BLOCK, (b + 1) * BLOCK)
            pieces = []
            for s in range(8):
                if b < 2:
                    px, py, p = 2 * b + s // 4, s % 4, 0
                else:
                    py, px, p = 2 * (b - 2) + s // 4, s % 4, 1
                pieces.append(g_full[py, 2 * px + m, p])
            g = jnp.concatenate(pieces, axis=1)
            moment = l_mc[m, :, cs].astype(F32) * l_ms[m, :, b:b + 1]
            second = l_vc[m, :, cs].astype(F32) * l_vs[m, :, b:b + 1]
            m2, v2, fresh = adam(moment, second, clip * g, l_master[m, :, cs])
            m_top = jnp.max(jnp.abs(m2), axis=1, keepdims=True) + 1e-20
            v_top = jnp.max(jnp.abs(v2), axis=1, keepdims=True) + 1e-20
            r_master[m, :, cs] = fresh
            r_mc[m, :, cs] = (m2 / m_top).astype(BF16)
            r_vc[m, :, cs] = (v2 / v_top).astype(BF16)
            tops_m = jnp.where(lane4 == b, m_top, tops_m)
            tops_v = jnp.where(lane4 == b, v_top, tops_v)
        r_ms[m] = tops_m
        r_vs[m] = tops_v
    outs = [
        local(a, b)
        for a, b in (
            (r_master, o_master), (r_mc, o_mc), (r_vc, o_vc), (r_ms, o_ms), (r_vs, o_vs),
        )
    ]

    to_pair, to_out = [], []
    rows_half = (pl.ds(0, V // 2), pl.ds(V // 2, V // 2))

    def finished(p, i, j):
        ref = wbuf.at[c, :, block_of(p, i, j)]
        to_pair.append((send(ref, ref, c=other), wbuf.at[other, :, block_of(p, i, j)],
                        o_w.at[other, :, block_of(p, i, j)]))
        to_out.append(local(ref, o_w.at[c, :, block_of(p, i, j)]))

    def spread(p, i, j, axis, targets):
        ref = wbuf.at[c, :, block_of(p, i, j)]
        return [send(ref, ref, **{axis: targets[side]}) for side in range(2)]

    def forward(p, i, j, axis, target, h):
        ref = wbuf.at[c, rows_half[h], block_of(p, i, j)]
        return send(ref, ref, **{axis: target})

    second_axis, first_axis, fwd2 = [None] * 2, [[None] * 4 for _ in range(2)], [None] * 2
    for p in range(2):
        a1, i1, a2, i2 = axes[p]
        for copy in ag1[p]:
            copy.wait_recv()
        second_axis[p] = spread(p, i1, i2, a2, roles2[p])
        first_axis[p][0] = spread(p, i1, i2, a1, roles[p])
        finished(p, i1, i2)
    for p in range(2):
        a1, i1, a2, i2 = axes[p]
        right2, left2, _, opp2 = roles2[p]
        fwd2[p] = []
        for side, origin in ((0, left2), (1, right2)):
            second_axis[p][side].wait_recv()
            fwd2[p].append(forward(p, i1, origin, a2, roles2[p][side], side))
            first_axis[p][1 + side] = spread(p, i1, origin, a1, roles[p])
            finished(p, i1, origin)

    fwd1 = [[None] * 4 for _ in range(2)]

    def pass_on(p, s):
        a1, i1, a2, i2 = axes[p]
        right1, left1, _, _ = roles[p]
        right2, left2, _, opp2 = roles2[p]
        j = (i2, left2, right2, opp2)[s]
        fwd1[p][s] = []
        for side, origin in ((0, left1), (1, right1)):
            first_axis[p][s][side].wait_recv()
            fwd1[p][s].append(forward(p, origin, j, a1, roles[p][side], side))
            finished(p, origin, j)

    def complete(p, s):
        a1, i1, a2, i2 = axes[p]
        right2, left2, _, opp2 = roles2[p]
        j = (i2, left2, right2, opp2)[s]
        for copy in fwd1[p][s]:
            copy.wait_recv()
        finished(p, roles[p][3], j)

    for p in range(2):
        pass_on(p, 0)
    for p in range(2):
        a1, i1, a2, i2 = axes[p]
        for copy in fwd2[p]:
            copy.wait_recv()
        first_axis[p][3] = spread(p, i1, roles2[p][3], a1, roles[p])
        finished(p, i1, roles2[p][3])
    for s in range(1, 4):
        for p in range(2):
            pass_on(p, s)
            complete(p, s - 1)
    for p in range(2):
        complete(p, 3)

    for copy, src, dst in to_pair:
        copy.wait_recv()
        to_out.append(local(src, dst))
    for copy in to_out + outs:
        copy.wait()
    for copy in started:
        copy.wait_send()
    assert counts[0] <= SEMS and counts[1] <= 128, counts


def body(partials, master, m_codes, v_codes, m_scales, v_scales):
    any_spec = pl.BlockSpec(memory_space=pl.ANY)
    vmem = pltpu.VMEM
    return pl.pallas_call(
        kernel,
        out_shape=(
            jax.ShapeDtypeStruct(master.shape, F32),
            jax.ShapeDtypeStruct(master.shape, BF16),
            jax.ShapeDtypeStruct(master.shape, BF16),
            jax.ShapeDtypeStruct(m_scales.shape, F32),
            jax.ShapeDtypeStruct(m_scales.shape, F32),
            jax.ShapeDtypeStruct((2, V, D), BF16),
        ),
        in_specs=[any_spec] * 6,
        out_specs=(any_spec,) * 6,
        scratch_shapes=[
            vmem((2, 3, V, WIDE), BF16),
            vmem((2, 3, V, WIDE), BF16),
            vmem((2, 2, 2, V, WIDE // 2), BF16),
            vmem((2, 2, V, WIDE), F32),
            vmem((2, 2, V, WIDE), F32),
            vmem((2, V, WIDE), F32),
            vmem((2, 2, V, SUB // 2), F32),
            vmem((2, 2, V, SUB // 2), F32),
            vmem((2, 2, 2, V, SUB // 2), F32),
            vmem((2, V, SUB), F32),
            vmem((2, 8, TILE, SUB), F32),
            vmem((2, TILE, SUB), F32),
            vmem((8, 8, 128), F32),
            vmem((8, 8, 128), F32),
            vmem((4, 8, 128), F32),
            vmem((8, 2, 2, SUB), F32),
            vmem((8, 2, 2, SUB), BF16),
            vmem((8, 2, 2, SUB), BF16),
            vmem((8, 4, 128), F32),
            vmem((2, 4, 128), F32),
            vmem((2, TILE, SUB), F32),
            vmem((2, TILE, SUB), F32),
            vmem((2, TILE, SUB), F32),
            vmem((8, 2, 2, SUB), F32),
            vmem((8, 2, 2, SUB), F32),
            vmem((4, 8, 2, 2, SUB), F32),
            vmem((2, V, D), BF16),
            vmem((2, 2, D), F32),
            vmem((2, 2, D), BF16),
            vmem((2, 2, D), BF16),
            vmem((2, 2, 4), F32),
            vmem((2, 2, 4), F32),
            vmem((2, 2, D), F32),
            vmem((2, 2, D), BF16),
            vmem((2, 2, D), BF16),
            vmem((2, 2, 4), F32),
            vmem((2, 2, 4), F32),
            pltpu.SemaphoreType.DMA((SEMS,)),
            pltpu.SemaphoreType.DMA((SEMS,)),
            pltpu.SemaphoreType.DMA((128,)),
        ],
        compiler_params=pltpu.CompilerParams(
            collective_id=0, has_side_effects=True, vmem_limit_bytes=48 * 1024 * 1024
        ),
        name="step",
    )(partials, master, m_codes, v_codes, m_scales, v_scales)


def solution(mesh):
    finer = Mesh(mesh.devices.reshape(NZ, NX, NC, NY), ("z", "x", "c", "y"))
    rows = P(None, ("z", "x", "c"), None)
    return jax.shard_map(
        body,
        mesh=finer,
        in_specs=(P("y", ("z", "x", "c"), None, None, None),) + (rows,) * 5,
        out_specs=(rows,) * 5 + (P(),),
        check_vma=False,
    )
```

```python
import functools

import jax
import jax.numpy as jnp
from jax import lax
from jax.experimental import pallas as pl
from jax.experimental.pallas import tpu as pltpu
from jax.sharding import Mesh
from jax.sharding import PartitionSpec as P

BLOCK = 2048
STEP = 10
MESH = pl.DeviceIdType.MESH
F32 = jnp.float32
BF16 = jnp.bfloat16

V = 128
D = 8192
HALF = 4096
WIDE = 1024
SUB = 256
NX, NY, NZ, NC = 4, 4, 8, 2
TILE = 16
SEMS = 256


def mod(a, n):
    return lax.rem(a + n, n)


def col(value, step):
    return pl.multiple_of(value, step)


def adam(moment, second, scaled, master):
    m2 = 0.9 * moment + 0.1 * scaled
    v2 = 0.95 * second + 0.05 * scaled * scaled
    update = m2 / (1.0 - 0.9**STEP) / (jnp.sqrt(v2 / (1.0 - 0.95**STEP)) + 1e-08)
    return m2, v2, master - 0.01 * update


def kernel(
    part_in, master_in, mc_in, vc_in, ms_in, vs_in,
    o_master, o_mc, o_vc, o_ms, o_vs, o_w,
    own, par, rcv1, snd, rcv2, s_buf, p2a, p2s, p2f, t_buf, z_buf, g_buf,
    nz, nxc, ny,
    e_master, e_mc, e_vc, e_s, sc_stage, mt, vt, wt,
    q_s, q_r, g_full,
    l_master, l_mc, l_vc, l_ms, l_vs,
    ssem, rsem, lsem,
):
    x, y, z, c = (lax.axis_index(a) for a in ("x", "y", "z", "c"))
    other = 1 - c
    started, counts = [], [0, 0]


    def send(src, dst, **dev):
        k = counts[0]
        counts[0] += 1
        copy = pltpu.make_async_remote_copy(
            src_ref=src, dst_ref=dst, send_sem=ssem.at[k], recv_sem=rsem.at[k],
            device_id=dev, device_id_type=MESH,
        )
        copy.start()
        started.append(copy)
        return copy

    def local(src, dst):
        k = counts[1]
        counts[1] += 1
        copy = pltpu.make_async_copy(src, dst, lsem.at[k])
        copy.start()
        return copy

    axes = (("x", x, "y", y), ("y", y, "x", x))
    roles = [tuple(mod(i + d, 4) for d in (1, -1, 0, 2)) for _, i, _, _ in axes]
    roles2 = [tuple(mod(j + d, 4) for d in (1, -1, 0, 2)) for _, _, _, j in axes]
    own_k = 2 * x + c

    own_loads = [[None] * 3 for _ in range(2)]
    for role in range(3):
        for p in range(2):
            cols = pl.ds(col(p * HALF + roles[p][role] * WIDE, WIDE), WIDE)
            own_loads[p][role] = local(part_in.at[0, 0, c, :, cols], own.at[p, role])
    state_loads = [
        local(a, b)
        for a, b in (
            (ms_in, l_ms), (vs_in, l_vs), (master_in, l_master), (mc_in, l_mc), (vc_in, l_vc),
        )
    ]

    barrier = pltpu.get_barrier_semaphore()
    peers = []
    for d in range(1, 8):
        k = mod(own_k + d, 8)
        peers.append({"x": k // 2, "c": lax.rem(k, 2)})
    for d in range(1, 4):
        peers.append({"y": mod(y + d, 4)})
    for d in (1, -1):
        peers.append({"y": mod(y + d, 4), "c": other})
    for d in range(1, 8):
        peers.append({"z": mod(z + d, 8)})
    for dev in peers:
        pl.semaphore_signal(barrier, inc=1, device_id=dev, device_id_type=MESH)
    pl.semaphore_wait(barrier, len(peers))

    raw = [[[None] * 2 for _ in range(2)] for _ in range(2)]
    for q in range(2):
        m = lax.rem(c + q, 2)
        for p in range(2):
            axis = axes[p][0]
            for h in range(2):
                cols = pl.ds(col(p * HALF + roles[p][3] * WIDE + h * (WIDE // 2), WIDE // 2), WIDE // 2)
                raw[p][h][q] = send(
                    part_in.at[0, 0, m, :, cols], rcv1.at[p, h, q], **{axis: roles[p][h], "c": m}
                )
    pair = [[None] * 3 for _ in range(2)]
    for role in range(3):
        for p in range(2):
            cols = pl.ds(col(p * HALF + roles[p][role] * WIDE, WIDE), WIDE)
            pair[p][role] = send(part_in.at[0, 0, other, :, cols], par.at[p, role], c=other)

    ex = []
    tile_cols = [
        lambda kx: col(kx * WIDE + y * SUB, SUB),
        lambda kx: col(HALF + y * WIDE + kx * SUB, SUB),
    ]
    for d in range(8):
        k = mod(own_k + d, 8)
        kx, kc = k // 2, lax.rem(k, 2)
        for src, dst in ((master_in, e_master), (mc_in, e_mc), (vc_in, e_vc)):
            for p in range(2):
                s = src.at[kc, :, pl.ds(tile_cols[p](kx), SUB)]
                t = dst.at[own_k, p]
                if d == 0:
                    ex.append(local(s, t))
                else:
                    ex.append(send(s, t, x=kx, c=kc))

    plain = [[None] * 2 for _ in range(2)]
    for p in range(2):
        axis = axes[p][0]
        for side in range(2):
            own_loads[p][side].wait()
            pair[p][side].wait_recv()
            h = 1 - side
            lo = h * (WIDE // 2)

            @pl.loop(0, V // TILE)
            def _(t):
                rows = pl.ds(pl.multiple_of(t * TILE, TILE), TILE)
                cc = pl.ds(lo, WIDE // 2)
                snd[p, side, rows, cc] = own[p, side, rows, cc].astype(F32) + par[p, side, rows, cc].astype(F32)

            cc = pl.ds(lo, WIDE // 2)
            plain[p][side] = send(snd.at[p, side, :, cc], rcv2.at[p, side, :, cc], **{axis: roles[p][side]})

    for load in state_loads:
        load.wait()
    sc_stage[...] = jnp.zeros_like(sc_stage)
    for m in range(2):
        sc_stage[m, 0:2, 0:4] = l_ms[m]
        sc_stage[m, 2:4, 0:4] = l_vs[m]
    e_s[own_k] = sc_stage[c]
    for d in range(1, 8):
        k = mod(own_k + d, 8)
        kx, kc = k // 2, lax.rem(k, 2)
        ex.append(send(sc_stage.at[kc], e_s.at[own_k], x=kx, c=kc))

    relay = [[None] * 2 for _ in range(2)]
    for p in range(2):
        axis = axes[p][0]
        for side in range(2):
            h = side
            lo = h * (WIDE // 2)
            for q in range(2):
                raw[p][h][q].wait_recv()

            @pl.loop(0, V // TILE)
            def _(t):
                rows = pl.ds(pl.multiple_of(t * TILE, TILE), TILE)
                cc = pl.ds(lo, WIDE // 2)
                near = own[p, side, rows, cc].astype(F32) + par[p, side, rows, cc].astype(F32)
                far = rcv1[p, h, 0, rows, :].astype(F32) + rcv1[p, h, 1, rows, :].astype(F32)
                snd[p, side, rows, cc] = near + far

            cc = pl.ds(lo, WIDE // 2)
            relay[p][side] = send(snd.at[p, side, :, cc], rcv2.at[p, side, :, cc], **{axis: roles[p][side]})

    for copy in ex:
        copy.wait_recv()
    blocks = (x // 2, 2 + y // 2)
    for k in range(8):
        e = e_s[k]
        lane = lax.broadcasted_iota(jnp.int32, e.shape, 1)
        for p in range(2):
            scale = jnp.sum(jnp.where(lane == blocks[p], e, 0.0), axis=1, keepdims=True)
            rows = pl.ds(2 * k, 2)
            mt[p, rows, :] = e_mc[k, p].astype(F32) * scale[0:2]
            vt[p, rows, :] = e_vc[k, p].astype(F32) * scale[2:4]
            wt[p, rows, :] = e_master[k, p]

    half = SUB // 2
    for p in range(2):
        axis2 = axes[p][2]
        own_loads[p][2].wait()
        pair[p][2].wait_recv()
        for side in range(2):
            plain[p][side].wait_recv()
            relay[p][side].wait_recv()

        @pl.loop(0, V // TILE)
        def _(t):
            rows = pl.ds(pl.multiple_of(t * TILE, TILE), TILE)
            near = own[p, 2, rows, :].astype(F32) + par[p, 2, rows, :].astype(F32)
            s_buf[p, rows, :] = near + rcv2[p, 0, rows, :] + rcv2[p, 1, rows, :]

    first2 = [[None] * 2 for _ in range(2)]
    plain2 = [[None] * 2 for _ in range(2)]
    relay2 = [[None] * 2 for _ in range(2)]
    for p in range(2):
        axis2 = axes[p][2]
        r2 = roles2[p]
        for h in range(2):
            cols = pl.ds(col(r2[3] * SUB + h * half, half), half)
            first2[p][h] = send(s_buf.at[p, :, cols], p2a.at[p, h], **{axis2: r2[h]})
        for side in range(2):
            h = 1 - side
            cols = pl.ds(col(r2[side] * SUB + h * half, half), half)
            plain2[p][side] = send(s_buf.at[p, :, cols], p2f.at[p, side, h], **{axis2: r2[side]})
    for p in range(2):
        axis2 = axes[p][2]
        r2 = roles2[p]
        for side in range(2):
            h = side
            cols = pl.ds(col(r2[side] * SUB + h * half, half), half)
            first2[p][h].wait_recv()
            p2s[p, side] = s_buf[p, :, cols] + p2a[p, h]
            relay2[p][side] = send(p2s.at[p, side], p2f.at[p, side, h], **{axis2: r2[side]})
    zc = [[None] * 8 for _ in range(2)]
    for p in range(2):
        r2 = roles2[p]
        for side in range(2):
            plain2[p][side].wait_recv()
            relay2[p][side].wait_recv()
        for h in range(2):
            cols = pl.ds(col(r2[2] * SUB + h * half, half), half)
            t_buf[p, :, h * half:(h + 1) * half] = s_buf[p, :, cols] + p2f[p, 0, h] + p2f[p, 1, h]
        for d in (4, 3, 5, 2, 6, 1, 7):
            zd = mod(z + d, 8)
            rows = pl.ds(pl.multiple_of(zd * TILE, TILE), TILE)
            zc[p][d] = send(t_buf.at[p, rows, :], z_buf.at[p, d], z=zd)

    my_rows = pl.ds(pl.multiple_of(z * TILE, TILE), TILE)
    square = jnp.zeros((8, 128), F32)
    for p in range(2):
        g = t_buf[p, my_rows, :]
        for d in range(1, 8):
            zc[p][d].wait_recv()
            g = g + z_buf[p, d]
        g_buf[p] = g
        sq = g * g
        for i in range(2):
            for j in range(2):
                square = square + sq[8 * i:8 * i + 8, 128 * j:128 * j + 128]
    nz[z] = square
    n1 = [send(nz.at[z], nz.at[z], z=mod(z + d, 8)) for d in (4, 3, 5, 2, 6, 1, 7)]

    for p in range(2):
        for k in range(8):
            q_s[k, p] = g_buf[p, 2 * k:2 * k + 2, :]
    q1 = []
    for d in range(1, 8):
        k = mod(own_k + d, 8)
        q1.append(send(q_s.at[k], q_r.at[own_k], x=k // 2, c=lax.rem(k, 2)))
    q_r[own_k] = q_s[own_k]

    for copy in n1:
        copy.wait_recv()
    nxc[own_k] = functools.reduce(lambda a, b: a + b, [nz[k] for k in range(8)])
    n2 = []
    for d in range(1, 8):
        k = mod(own_k + d, 8)
        n2.append(send(nxc.at[own_k], nxc.at[own_k], x=k // 2, c=lax.rem(k, 2)))

    for copy in q1:
        copy.wait_recv()
    q2 = [send(q_r, g_full.at[y], y=mod(y + d, 4)) for d in range(1, 4)]
    g_full[y] = q_r[...]

    for copy in n2:
        copy.wait_recv()
    ny[y] = functools.reduce(lambda a, b: a + b, [nxc[k] for k in range(8)])
    n3 = [send(ny.at[y], ny.at[y], y=mod(y + d, 4)) for d in (2, 1, 3)]
    for copy in n3:
        copy.wait_recv()
    total = functools.reduce(lambda a, b: a + b, [ny[k] for k in range(4)])
    total = jnp.sum(jnp.sum(total, axis=1, keepdims=True), axis=0, keepdims=True)
    clip = 1.0 / jnp.maximum(jnp.sqrt(total), 1.0)

    block_of = lambda p, i, j: pl.ds(col(p * HALF + i * WIDE + j * SUB, SUB), SUB)
    for p in range(2):
        i1, i2 = axes[p][1], axes[p][3]
        _, _, fresh = adam(mt[p], vt[p], clip * g_buf[p], wt[p])
        o_w[c, my_rows, block_of(p, i1, i2)] = fresh.astype(BF16)
    ag1 = [[], []]
    for d in (4, 3, 5, 2, 6, 1, 7):
        for p in range(2):
            ref = o_w.at[c, my_rows, block_of(p, axes[p][1], axes[p][3])]
            ag1[p].append(send(ref, ref, z=mod(z + d, 8)))

    for copy in q2:
        copy.wait_recv()
    lane4 = lax.broadcasted_iota(jnp.int32, (2, 4), 1)
    for m in range(2):
        tops_m = jnp.zeros((2, 4), F32)
        tops_v = jnp.zeros((2, 4), F32)
        for b in range(4):
            cs = slice(b * BLOCK, (b + 1) * BLOCK)
            pieces = []
            for s in range(8):
                if b < 2:
                    px, py, p = 2 * b + s // 4, s % 4, 0
                else:
                    py, px, p = 2 * (b - 2) + s // 4, s % 4, 1
                pieces.append(g_full[py, 2 * px + m, p])
            g = jnp.concatenate(pieces, axis=1)
            moment = l_mc[m, :, cs].astype(F32) * l_ms[m, :, b:b + 1]
            second = l_vc[m, :, cs].astype(F32) * l_vs[m, :, b:b + 1]
            m2, v2, fresh = adam(moment, second, clip * g, l_master[m, :, cs])
            m_top = jnp.max(jnp.abs(m2), axis=1, keepdims=True) + 1e-20
            v_top = jnp.max(jnp.abs(v2), axis=1, keepdims=True) + 1e-20
            o_master[m, :, cs] = fresh
            o_mc[m, :, cs] = (m2 / m_top).astype(BF16)
            o_vc[m, :, cs] = (v2 / v_top).astype(BF16)
            tops_m = jnp.where(lane4 == b, m_top, tops_m)
            tops_v = jnp.where(lane4 == b, v_top, tops_v)
        o_ms[m] = tops_m
        o_vs[m] = tops_v

    to_pair = []
    rows_half = (pl.ds(0, V // 2), pl.ds(V // 2, V // 2))

    def finished(p, i, j):
        ref = o_w.at[c, :, block_of(p, i, j)]
        to_pair.append(send(ref, ref, c=other))

    def spread(p, i, j, axis, targets):
        ref = o_w.at[c, :, block_of(p, i, j)]
        return [send(ref, ref, **{axis: targets[side]}) for side in range(2)]

    def forward(p, i, j, axis, target, h):
        ref = o_w.at[c, rows_half[h], block_of(p, i, j)]
        return send(ref, ref, **{axis: target})

    second_axis, first_axis, fwd2 = [None] * 2, [[None] * 4 for _ in range(2)], [None] * 2
    for p in range(2):
        a1, i1, a2, i2 = axes[p]
        for copy in ag1[p]:
            copy.wait_recv()
        second_axis[p] = spread(p, i1, i2, a2, roles2[p])
        first_axis[p][0] = spread(p, i1, i2, a1, roles[p])
        finished(p, i1, i2)
    for p in range(2):
        a1, i1, a2, i2 = axes[p]
        right2, left2, _, opp2 = roles2[p]
        fwd2[p] = []
        for side, origin in ((0, left2), (1, right2)):
            second_axis[p][side].wait_recv()
            fwd2[p].append(forward(p, i1, origin, a2, roles2[p][side], side))
            first_axis[p][1 + side] = spread(p, i1, origin, a1, roles[p])
            finished(p, i1, origin)

    fwd1 = [[None] * 4 for _ in range(2)]

    def pass_on(p, s):
        a1, i1, a2, i2 = axes[p]
        right1, left1, _, _ = roles[p]
        right2, left2, _, opp2 = roles2[p]
        j = (i2, left2, right2, opp2)[s]
        fwd1[p][s] = []
        for side, origin in ((0, left1), (1, right1)):
            first_axis[p][s][side].wait_recv()
            fwd1[p][s].append(forward(p, origin, j, a1, roles[p][side], side))
            finished(p, origin, j)

    def complete(p, s):
        a1, i1, a2, i2 = axes[p]
        right2, left2, _, opp2 = roles2[p]
        j = (i2, left2, right2, opp2)[s]
        for copy in fwd1[p][s]:
            copy.wait_recv()
        finished(p, roles[p][3], j)

    for p in range(2):
        pass_on(p, 0)
    for p in range(2):
        a1, i1, a2, i2 = axes[p]
        for copy in fwd2[p]:
            copy.wait_recv()
        first_axis[p][3] = spread(p, i1, roles2[p][3], a1, roles[p])
        finished(p, i1, roles2[p][3])
    for s in range(1, 4):
        for p in range(2):
            pass_on(p, s)
            complete(p, s - 1)
    for p in range(2):
        complete(p, 3)

    for copy in to_pair:
        copy.wait_recv()
    for copy in started:
        copy.wait_send()
    assert counts[0] <= SEMS and counts[1] <= 128, counts


def write_out(*refs):
    sems = refs[12]
    copies = [pltpu.make_async_copy(refs[k], refs[k + 6], sems.at[k]) for k in (5, 0, 1, 2, 3, 4)]
    for copy in copies:
        copy.start()
    for copy in copies:
        copy.wait()


def body(partials, master, m_codes, v_codes, m_scales, v_scales):
    any_spec = pl.BlockSpec(memory_space=pl.ANY)
    vmem = pltpu.VMEM
    small = [pltpu.with_memory_space_constraint(a, pltpu.HBM) for a in (master, m_codes, v_codes, m_scales, v_scales)]
    results = pl.pallas_call(
        kernel,
        out_shape=(
            jax.ShapeDtypeStruct(master.shape, F32),
            jax.ShapeDtypeStruct(master.shape, BF16),
            jax.ShapeDtypeStruct(master.shape, BF16),
            jax.ShapeDtypeStruct(m_scales.shape, F32),
            jax.ShapeDtypeStruct(m_scales.shape, F32),
            jax.ShapeDtypeStruct((2, V, D), BF16),
        ),
        in_specs=[pl.BlockSpec(memory_space=pltpu.HBM)] * 6,
        out_specs=(pl.BlockSpec(memory_space=pltpu.VMEM),) * 6,
        scratch_shapes=[
            vmem((2, 3, V, WIDE), BF16),
            vmem((2, 3, V, WIDE), BF16),
            vmem((2, 2, 2, V, WIDE // 2), BF16),
            vmem((2, 2, V, WIDE), F32),
            vmem((2, 2, V, WIDE), F32),
            vmem((2, V, WIDE), F32),
            vmem((2, 2, V, SUB // 2), F32),
            vmem((2, 2, V, SUB // 2), F32),
            vmem((2, 2, 2, V, SUB // 2), F32),
            vmem((2, V, SUB), F32),
            vmem((2, 8, TILE, SUB), F32),
            vmem((2, TILE, SUB), F32),
            vmem((8, 8, 128), F32),
            vmem((8, 8, 128), F32),
            vmem((4, 8, 128), F32),
            vmem((8, 2, 2, SUB), F32),
            vmem((8, 2, 2, SUB), BF16),
            vmem((8, 2, 2, SUB), BF16),
            vmem((8, 4, 128), F32),
            vmem((2, 4, 128), F32),
            vmem((2, TILE, SUB), F32),
            vmem((2, TILE, SUB), F32),
            vmem((2, TILE, SUB), F32),
            vmem((8, 2, 2, SUB), F32),
            vmem((8, 2, 2, SUB), F32),
            vmem((4, 8, 2, 2, SUB), F32),
            vmem((2, 2, D), F32),
            vmem((2, 2, D), BF16),
            vmem((2, 2, D), BF16),
            vmem((2, 2, 4), F32),
            vmem((2, 2, 4), F32),
            pltpu.SemaphoreType.DMA((SEMS,)),
            pltpu.SemaphoreType.DMA((SEMS,)),
            pltpu.SemaphoreType.DMA((128,)),
        ],
        compiler_params=pltpu.CompilerParams(
            collective_id=0, has_side_effects=True, vmem_limit_bytes=48 * 1024 * 1024
        ),
        name="step",
    )(partials, *small)
    return pl.pallas_call(
        write_out,
        out_shape=tuple(jax.ShapeDtypeStruct(a.shape, a.dtype) for a in results),
        in_specs=[any_spec] * 6,
        out_specs=(any_spec,) * 6,
        scratch_shapes=[pltpu.SemaphoreType.DMA((6,))],
        compiler_params=pltpu.CompilerParams(vmem_limit_bytes=1024 * 1024),
        name="write_out",
    )(*results)


def solution(mesh):
    finer = Mesh(mesh.devices.reshape(NZ, NX, NC, NY), ("z", "x", "c", "y"))
    rows = P(None, ("z", "x", "c"), None)
    return jax.shard_map(
        body,
        mesh=finer,
        in_specs=(P("y", ("z", "x", "c"), None, None, None),) + (rows,) * 5,
        out_specs=(rows,) * 5 + (P(),),
        check_vma=False,
    )
```

```python
import functools
import math

import jax
import jax.numpy as jnp
from jax import lax
from jax.experimental import pallas as pl
from jax.experimental.pallas import tpu as pltpu
from jax.sharding import Mesh
from jax.sharding import PartitionSpec as P

BLOCK = 2048
STEP = 10
MESH = pl.DeviceIdType.MESH
F32 = jnp.float32
BF16 = jnp.bfloat16

V = 128
D = 8192
HALF = 4096
WIDE = 1024
SUB = 256
NX, NY, NZ, NC = 4, 4, 8, 2
TILE = 16
SEMS = 80
LOCAL_SEMS = 18
LIMIT_KIB = 12 * 1024


def mod(a, n):
    return lax.rem(a + n, n)


def col(value, step):
    return pl.multiple_of(value, step)


def adam(moment, second, scaled, master):
    m2 = 0.9 * moment + 0.1 * scaled
    v2 = 0.95 * second + 0.05 * scaled * scaled
    update = m2 / (1.0 - 0.9**STEP) / (jnp.sqrt(v2 / (1.0 - 0.95**STEP)) + 1e-08)
    return m2, v2, master - 0.01 * update


def kernel(
    part_in, master_in, mc_in, vc_in, ms_in, vs_in,
    o_master, o_mc, o_vc, o_ms, o_vs, o_w,
    own, par, rcv1, snd, rcv2, s_buf, p2f, t_buf, z_buf, g_buf,
    nzc, nxy,
    e_master, e_mc, e_vc, e_s, sc_stage, mt, vt, wt,
    q_s, q_r, g_full,
    l_master, l_mc, l_vc, l_ms, l_vs, bytes_ref,
    ssem, rsem, lsem,
):
    x, y, z, c = (lax.axis_index(a) for a in ("x", "y", "z", "c"))
    other = 1 - c
    groups, sent = [0, 0], [0]

    def size(ref):
        return math.prod(ref.shape) * ref.dtype.itemsize // 1024

    def group():
        groups[0] += 1
        return groups[0] - 1

    def send(src, dst, k, **dev):
        sent[0] += size(src)
        pltpu.make_async_remote_copy(
            src_ref=src, dst_ref=dst, send_sem=ssem.at[0], recv_sem=rsem.at[k],
            device_id=dev, device_id_type=MESH,
        ).start()

    def arrived(k, kib):
        ref = bytes_ref.at[pl.ds(0, kib)]
        pltpu.make_async_copy(ref, ref, rsem.at[k]).wait()

    def all_sent():
        assert sent[0] <= LIMIT_KIB
        ref = bytes_ref.at[pl.ds(0, sent[0])]
        pltpu.make_async_copy(ref, ref, ssem.at[0]).wait()


    def local(src, dst):
        groups[1] += 1
        copy = pltpu.make_async_copy(src, dst, lsem.at[groups[1] - 1])
        copy.start()
        return copy


    axes = (("x", x, "y", y), ("y", y, "x", x))
    roles = [tuple(mod(i + d, 4) for d in (1, -1, 0, 2)) for _, i, _, _ in axes]
    roles2 = [tuple(mod(j + d, 4) for d in (1, -1, 0, 2)) for _, _, _, j in axes]
    own_k = 2 * x + c

    own_loads = [[None] * 3 for _ in range(2)]
    for role in range(3):
        for p in range(2):
            cols = pl.ds(col(p * HALF + roles[p][role] * WIDE, WIDE), WIDE)
            own_loads[p][role] = local(part_in.at[0, 0, c, :, cols], own.at[p, role])
    state_loads = [
        local(a, b)
        for a, b in (
            (ms_in, l_ms), (vs_in, l_vs), (master_in, l_master), (mc_in, l_mc), (vc_in, l_vc),
        )
    ]

    barrier = pltpu.get_barrier_semaphore()
    xc_peers, xy_peers, zc_peers = [], [], []
    for d in range(1, 8):
        k = mod(own_k + d, 8)
        xc_peers.append((k, {"x": k // 2, "c": lax.rem(k, 2)}))
    for d in (10, 9, 11, 6, 14, 2, 8, 5, 7, 13, 15, 1, 3, 4, 12):
        xy_peers.append({"x": mod(x + d // 4, 4), "y": mod(y + d % 4, 4)})
    for d in (8, 9, 6, 7, 10, 11, 4, 5, 12, 13, 2, 3, 14, 15, 1):
        zc_peers.append({"z": mod(z + d // 2, 8), "c": lax.rem(c + d % 2, 2)})
    greeted = list(xy_peers) + list(zc_peers)
    greeted += [{"x": mod(x + d, 4), "c": other} for d in (1, 2, 3)]
    greeted += [{"y": mod(y + d, 4), "c": other} for d in (1, 3)]
    for dev in greeted:
        pl.semaphore_signal(barrier, inc=1, device_id=dev, device_id_type=MESH)
    pl.semaphore_wait(barrier, len(greeted))

    raw = [[group() for _ in range(2)] for _ in range(2)]
    for q in range(2):
        m = lax.rem(c + q, 2)
        for p in range(2):
            axis = axes[p][0]
            for h in range(2):
                cols = pl.ds(col(p * HALF + roles[p][3] * WIDE + h * (WIDE // 2), WIDE // 2), WIDE // 2)
                send(part_in.at[0, 0, m, :, cols], rcv1.at[p, h, q], raw[p][h], **{axis: roles[p][h], "c": m})
    pair = [[group() for _ in range(3)] for _ in range(2)]
    for role in range(3):
        for p in range(2):
            cols = pl.ds(col(p * HALF + roles[p][role] * WIDE, WIDE), WIDE)
            send(part_in.at[0, 0, other, :, cols], par.at[p, role], pair[p][role], c=other)

    from_side = [[group() for _ in range(2)] for _ in range(2)]
    for p in range(2):
        axis = axes[p][0]
        for side in range(2):
            own_loads[p][side].wait()
            arrived(pair[p][side], size(par.at[p, side]))
            lo = (1 - side) * (WIDE // 2)

            @pl.loop(0, V // TILE)
            def _(t):
                rows = pl.ds(pl.multiple_of(t * TILE, TILE), TILE)
                cc = pl.ds(lo, WIDE // 2)
                snd[p, side, rows, cc] = own[p, side, rows, cc].astype(F32) + par[p, side, rows, cc].astype(F32)

            cc = pl.ds(lo, WIDE // 2)
            send(snd.at[p, side, :, cc], rcv2.at[p, side, :, cc], from_side[p][side], **{axis: roles[p][side]})

    state = group()
    tile_cols = [
        lambda kx: col(kx * WIDE + y * SUB, SUB),
        lambda kx: col(HALF + y * WIDE + kx * SUB, SUB),
    ]
    own_state = []
    for src, dst in ((master_in, e_master), (mc_in, e_mc), (vc_in, e_vc)):
        for p in range(2):
            own_state.append(local(src.at[c, :, pl.ds(tile_cols[p](x), SUB)], dst.at[own_k, p]))
            for k, dev in xc_peers:
                send(src.at[dev["c"], :, pl.ds(tile_cols[p](dev["x"]), SUB)], dst.at[own_k, p], state, **dev)
    for load in state_loads:
        load.wait()
    sc_stage[...] = jnp.zeros_like(sc_stage)
    for m in range(2):
        sc_stage[m, 0:2, 0:4] = l_ms[m]
        sc_stage[m, 2:4, 0:4] = l_vs[m]
    e_s[own_k] = sc_stage[c]
    for k, dev in xc_peers:
        send(sc_stage.at[dev["c"]], e_s.at[own_k], state, **dev)

    for p in range(2):
        axis = axes[p][0]
        for side in range(2):
            h = side
            lo = h * (WIDE // 2)
            arrived(raw[p][h], size(rcv1.at[p, h]))

            @pl.loop(0, V // TILE)
            def _(t):
                rows = pl.ds(pl.multiple_of(t * TILE, TILE), TILE)
                cc = pl.ds(lo, WIDE // 2)
                near = own[p, side, rows, cc].astype(F32) + par[p, side, rows, cc].astype(F32)
                far = rcv1[p, h, 0, rows, :].astype(F32) + rcv1[p, h, 1, rows, :].astype(F32)
                snd[p, side, rows, cc] = near + far

            cc = pl.ds(lo, WIDE // 2)
            send(snd.at[p, side, :, cc], rcv2.at[p, side, :, cc], from_side[p][side], **{axis: roles[p][side]})

    for copy in own_state:
        copy.wait()
    arrived(state, 7 * 10)
    blocks = (x // 2, 2 + y // 2)
    for k in range(8):
        e = e_s[k]
        lane = lax.broadcasted_iota(jnp.int32, e.shape, 1)
        for p in range(2):
            scale = jnp.sum(jnp.where(lane == blocks[p], e, 0.0), axis=1, keepdims=True)
            rows = pl.ds(2 * k, 2)
            mt[p, rows, :] = e_mc[k, p].astype(F32) * scale[0:2]
            vt[p, rows, :] = e_vc[k, p].astype(F32) * scale[2:4]
            wt[p, rows, :] = e_master[k, p]

    second = [group() for _ in range(2)]
    for p in range(2):
        axis2, r2 = axes[p][2], roles2[p]
        own_loads[p][2].wait()
        arrived(pair[p][2], size(par.at[p, 2]))
        for side in range(2):
            arrived(from_side[p][side], size(rcv2.at[p, side]))
        for n in (3, 0, 1, 2):
            cols = pl.ds(col(r2[n] * SUB, SUB), SUB)

            @pl.loop(0, V // TILE)
            def _(t):
                rows = pl.ds(pl.multiple_of(t * TILE, TILE), TILE)
                near = own[p, 2, rows, cols].astype(F32) + par[p, 2, rows, cols].astype(F32)
                s_buf[p, rows, cols] = near + rcv2[p, 0, rows, cols] + rcv2[p, 1, rows, cols]

            if n != 2:
                send(s_buf.at[p, :, cols], p2f.at[p, n if n < 2 else 2], second[p], **{axis2: r2[n]})

    third = [group() for _ in range(2)]
    for p in range(2):
        r2 = roles2[p]
        arrived(second[p], size(p2f.at[p]))
        cols = pl.ds(col(r2[2] * SUB, SUB), SUB)

        @pl.loop(0, V // TILE)
        def _(t):
            rows = pl.ds(pl.multiple_of(t * TILE, TILE), TILE)
            t_buf[p, rows, :] = s_buf[p, rows, cols] + p2f[p, 0, rows] + (p2f[p, 1, rows] + p2f[p, 2, rows])

        for d in (4, 3, 5, 2, 6, 1, 7):
            zd = mod(z + d, 8)
            rows = pl.ds(pl.multiple_of(zd * TILE, TILE), TILE)
            send(t_buf.at[p, rows, :], z_buf.at[p, d - 1], third[p], z=zd)

    my_rows = pl.ds(pl.multiple_of(z * TILE, TILE), TILE)
    square = jnp.zeros((8, 128), F32)
    for p in range(2):
        arrived(third[p], size(z_buf.at[p]))
        g = t_buf[p, my_rows, :]
        for d in range(7):
            g = g + z_buf[p, d]
        g_buf[p] = g
        sq = g * g
        for i in range(2):
            for j in range(2):
                square = square + sq[8 * i:8 * i + 8, 128 * j:128 * j + 128]
    norm_zc, norm_xy, q1, q2 = (group() for _ in range(4))
    slot = 2 * z + c
    nzc[slot] = square
    for dev in zc_peers:
        send(nzc.at[slot], nzc.at[slot], norm_zc, **dev)

    for p in range(2):
        for k in range(8):
            q_s[k, p] = g_buf[p, 2 * k:2 * k + 2, :]
    for k, dev in xc_peers:
        send(q_s.at[k], q_r.at[own_k], q1, **dev)
    q_r[own_k] = q_s[own_k]

    arrived(norm_zc, 15 * 4)
    slot = 4 * x + y
    nxy[slot] = functools.reduce(lambda a, b: a + b, [nzc[k] for k in range(16)])
    for dev in xy_peers:
        send(nxy.at[slot], nxy.at[slot], norm_xy, **dev)

    arrived(q1, 7 * 4)
    for d in (2, 1, 3):
        send(q_r, g_full.at[y], q2, y=mod(y + d, 4))
    g_full[y] = q_r[...]

    arrived(norm_xy, 15 * 4)
    total = functools.reduce(lambda a, b: a + b, [nxy[k] for k in range(16)])
    total = jnp.sum(jnp.sum(total, axis=1, keepdims=True), axis=0, keepdims=True)
    clip = 1.0 / jnp.maximum(jnp.sqrt(total), 1.0)

    block_of = lambda p, i, j: pl.ds(col(p * HALF + i * WIDE + j * SUB, SUB), SUB)
    for p in range(2):
        i1, i2 = axes[p][1], axes[p][3]
        _, _, fresh = adam(mt[p], vt[p], clip * g_buf[p], wt[p])
        o_w[c, my_rows, block_of(p, i1, i2)] = fresh.astype(BF16)
    ag1 = [group() for _ in range(2)]
    for d in (4, 3, 5, 2, 6, 1, 7):
        for p in range(2):
            ref = o_w.at[c, my_rows, block_of(p, axes[p][1], axes[p][3])]
            send(ref, ref, ag1[p], z=mod(z + d, 8))

    arrived(q2, 3 * 32)
    lane4 = lax.broadcasted_iota(jnp.int32, (2, 4), 1)
    for m in range(2):
        tops_m = jnp.zeros((2, 4), F32)
        tops_v = jnp.zeros((2, 4), F32)
        for b in range(4):
            cs = slice(b * BLOCK, (b + 1) * BLOCK)
            pieces = []
            for s in range(8):
                if b < 2:
                    px, py, p = 2 * b + s // 4, s % 4, 0
                else:
                    py, px, p = 2 * (b - 2) + s // 4, s % 4, 1
                pieces.append(g_full[py, 2 * px + m, p])
            g = jnp.concatenate(pieces, axis=1)
            moment = l_mc[m, :, cs].astype(F32) * l_ms[m, :, b:b + 1]
            second_ = l_vc[m, :, cs].astype(F32) * l_vs[m, :, b:b + 1]
            m2, v2, fresh = adam(moment, second_, clip * g, l_master[m, :, cs])
            m_top = jnp.max(jnp.abs(m2), axis=1, keepdims=True) + 1e-20
            v_top = jnp.max(jnp.abs(v2), axis=1, keepdims=True) + 1e-20
            o_master[m, :, cs] = fresh
            o_mc[m, :, cs] = (m2 / m_top).astype(BF16)
            o_vc[m, :, cs] = (v2 / v_top).astype(BF16)
            tops_m = jnp.where(lane4 == b, m_top, tops_m)
            tops_v = jnp.where(lane4 == b, v_top, tops_v)
        o_ms[m] = tops_m
        o_vs[m] = tops_v

    to_pair = group()
    rows_half = (pl.ds(0, V // 2), pl.ds(V // 2, V // 2))
    block_kib = V * SUB * 2 // 1024

    def finished(p, i, j):
        ref = o_w.at[c, :, block_of(p, i, j)]
        send(ref, ref, to_pair, c=other)

    def spread(p, i, j, axis, targets):
        ref = o_w.at[c, :, block_of(p, i, j)]
        ks = [group() for _ in targets]
        for k, target in zip(ks, targets):
            send(ref, ref, k, **{axis: target})
        return ks

    def forward(p, i, j, axis, target, h, k):
        ref = o_w.at[c, rows_half[h], block_of(p, i, j)]
        send(ref, ref, k, **{axis: target})

    along2, along1 = [None] * 2, [[None] * 4 for _ in range(2)]
    for p in range(2):
        a1, i1, a2, i2 = axes[p]
        arrived(ag1[p], 7 * TILE * SUB * 2 // 1024)
        right2, left2, _, opp2 = roles2[p]
        along2[p] = spread(p, i1, i2, a2, (opp2, right2, left2))
        along1[p][0] = spread(p, i1, i2, a1, roles[p][:2])
        finished(p, i1, i2)
    for n, s in ((1, 1), (2, 2), (0, 3)):
        for p in range(2):
            a1, i1, a2, i2 = axes[p]
            right2, left2, _, opp2 = roles2[p]
            origin = (opp2, left2, right2)[n]
            arrived(along2[p][n], block_kib)
            targets = roles[p][:2] if s < 3 else (roles[p][3],) + roles[p][:2]
            along1[p][s] = spread(p, i1, origin, a1, targets)
            finished(p, i1, origin)

    fwd1 = [[group() for _ in range(3)] for _ in range(2)]

    def column(p, s):
        right2, left2, _, opp2 = roles2[p]
        return (axes[p][3], left2, right2, opp2)[s]

    def pass_on(p, s):
        right1, left1, _, _ = roles[p]
        for side, origin in ((0, left1), (1, right1)):
            arrived(along1[p][s][side], block_kib)
            forward(p, origin, column(p, s), axes[p][0], roles[p][side], side, fwd1[p][s])
            finished(p, origin, column(p, s))

    for s in range(3):
        for p in range(2):
            pass_on(p, s)
    for s in range(3):
        for p in range(2):
            arrived(fwd1[p][s], block_kib)
            finished(p, roles[p][3], column(p, s))
    for n, role in ((1, 1), (2, 0), (0, 3)):
        for p in range(2):
            arrived(along1[p][3][n], block_kib)
            finished(p, roles[p][role], column(p, 3))
    arrived(to_pair, size(o_w.at[0]))
    all_sent()
    assert groups[0] <= SEMS and groups[1] <= LOCAL_SEMS, (groups, sent)


def write_out(*refs):
    sems = refs[12]
    copies = [pltpu.make_async_copy(refs[k], refs[k + 6], sems.at[k]) for k in (5, 0, 1, 2, 3, 4)]
    for copy in copies:
        copy.start()
    for copy in copies:
        copy.wait()


def body(partials, master, m_codes, v_codes, m_scales, v_scales):
    any_spec = pl.BlockSpec(memory_space=pl.ANY)
    vmem = pltpu.VMEM
    small = [pltpu.with_memory_space_constraint(a, pltpu.HBM) for a in (master, m_codes, v_codes, m_scales, v_scales)]
    results = pl.pallas_call(
        kernel,
        out_shape=(
            jax.ShapeDtypeStruct(master.shape, F32),
            jax.ShapeDtypeStruct(master.shape, BF16),
            jax.ShapeDtypeStruct(master.shape, BF16),
            jax.ShapeDtypeStruct(m_scales.shape, F32),
            jax.ShapeDtypeStruct(m_scales.shape, F32),
            jax.ShapeDtypeStruct((2, V, D), BF16),
        ),
        in_specs=[pl.BlockSpec(memory_space=pltpu.HBM)] * 6,
        out_specs=(pl.BlockSpec(memory_space=pltpu.VMEM),) * 6,
        scratch_shapes=[
            vmem((2, 3, V, WIDE), BF16),
            vmem((2, 3, V, WIDE), BF16),
            vmem((2, 2, 2, V, WIDE // 2), BF16),
            vmem((2, 2, V, WIDE), F32),
            vmem((2, 2, V, WIDE), F32),
            vmem((2, V, WIDE), F32),
            vmem((2, 3, V, SUB), F32),
            vmem((2, V, SUB), F32),
            vmem((2, 7, TILE, SUB), F32),
            vmem((2, TILE, SUB), F32),
            vmem((16, 8, 128), F32),
            vmem((16, 8, 128), F32),
            vmem((8, 2, 2, SUB), F32),
            vmem((8, 2, 2, SUB), BF16),
            vmem((8, 2, 2, SUB), BF16),
            vmem((8, 4, 128), F32),
            vmem((2, 4, 128), F32),
            vmem((2, TILE, SUB), F32),
            vmem((2, TILE, SUB), F32),
            vmem((2, TILE, SUB), F32),
            vmem((8, 2, 2, SUB), F32),
            vmem((8, 2, 2, SUB), F32),
            vmem((4, 8, 2, 2, SUB), F32),
            vmem((2, 2, D), F32),
            vmem((2, 2, D), BF16),
            vmem((2, 2, D), BF16),
            vmem((2, 2, 4), F32),
            vmem((2, 2, 4), F32),
            vmem((LIMIT_KIB, 2, 128), F32),
            pltpu.SemaphoreType.DMA((1,)),
            pltpu.SemaphoreType.DMA((SEMS,)),
            pltpu.SemaphoreType.DMA((LOCAL_SEMS,)),
        ],
        compiler_params=pltpu.CompilerParams(
            collective_id=0, has_side_effects=True, vmem_limit_bytes=48 * 1024 * 1024
        ),
        name="step",
    )(partials, *small)
    return pl.pallas_call(
        write_out,
        out_shape=tuple(jax.ShapeDtypeStruct(a.shape, a.dtype) for a in results),
        in_specs=[any_spec] * 6,
        out_specs=(any_spec,) * 6,
        scratch_shapes=[pltpu.SemaphoreType.DMA((6,))],
        compiler_params=pltpu.CompilerParams(vmem_limit_bytes=1024 * 1024),
        name="write_out",
    )(*results)


def solution(mesh):
    finer = Mesh(mesh.devices.reshape(NZ, NX, NC, NY), ("z", "x", "c", "y"))
    rows = P(None, ("z", "x", "c"), None)
    return jax.shard_map(
        body,
        mesh=finer,
        in_specs=(P("y", ("z", "x", "c"), None, None, None),) + (rows,) * 5,
        out_specs=(rows,) * 5 + (P(),),
        check_vma=False,
    )
```

```python
import functools
import math

import jax
import jax.numpy as jnp
from jax import lax
from jax.experimental import pallas as pl
from jax.experimental.pallas import tpu as pltpu
from jax.sharding import Mesh
from jax.sharding import PartitionSpec as P

BLOCK = 2048
STEP = 10
MESH = pl.DeviceIdType.MESH
F32 = jnp.float32
BF16 = jnp.bfloat16

V = 128
D = 8192
HALF = 4096
WIDE = 1024
SUB = 256
NX, NY, NZ, NC = 4, 4, 8, 2
TILE = 16
SEMS = 80
LOCAL_SEMS = 18
LIMIT_KIB = 12 * 1024


def mod(a, n):
    return lax.rem(a + n, n)


def col(value, step):
    return pl.multiple_of(value, step)


def adam(moment, second, scaled, master):
    m2 = 0.9 * moment + 0.1 * scaled
    v2 = 0.95 * second + 0.05 * scaled * scaled
    update = m2 / (1.0 - 0.9**STEP) / (jnp.sqrt(v2 / (1.0 - 0.95**STEP)) + 1e-08)
    return m2, v2, master - 0.01 * update


def kernel(
    part_in, master_in, mc_in, vc_in, ms_in, vs_in,
    o_master, o_mc, o_vc, o_ms, o_vs, o_w,
    own, par, rcv1, snd, rcv2, s_buf, p2f, t_buf, z_buf, g_buf,
    nzc, nxy,
    e_master, e_mc, e_vc, e_s, sc_stage, tile, st, g_col,
    q_s, q_r, g_full,
    l_master, l_mc, l_vc, l_ms, l_vs, bytes_ref,
    ssem, rsem, lsem,
):
    x, y, z, c = (lax.axis_index(a) for a in ("x", "y", "z", "c"))
    other = 1 - c
    groups, sent = [0, 0], [0]

    def size(ref):
        return math.prod(ref.shape) * ref.dtype.itemsize // 1024

    def group():
        groups[0] += 1
        return groups[0] - 1

    def send(src, dst, k, **dev):
        sent[0] += size(src)
        pltpu.make_async_remote_copy(
            src_ref=src, dst_ref=dst, send_sem=ssem.at[0], recv_sem=rsem.at[k],
            device_id=dev, device_id_type=MESH,
        ).start()

    def arrived(k, kib):
        ref = bytes_ref.at[pl.ds(0, kib)]
        pltpu.make_async_copy(ref, ref, rsem.at[k]).wait()

    def all_sent():
        assert sent[0] <= LIMIT_KIB
        ref = bytes_ref.at[pl.ds(0, sent[0])]
        pltpu.make_async_copy(ref, ref, ssem.at[0]).wait()


    def local(src, dst):
        groups[1] += 1
        copy = pltpu.make_async_copy(src, dst, lsem.at[groups[1] - 1])
        copy.start()
        return copy


    axes = (("x", x, "y", y), ("y", y, "x", x))
    roles = [tuple(mod(i + d, 4) for d in (1, -1, 0, 2)) for _, i, _, _ in axes]
    roles2 = [tuple(mod(j + d, 4) for d in (1, -1, 0, 2)) for _, _, _, j in axes]
    own_k = 2 * x + c

    own_loads = [[None] * 3 for _ in range(2)]
    for role in range(3):
        for p in range(2):
            cols = pl.ds(col(p * HALF + roles[p][role] * WIDE, WIDE), WIDE)
            own_loads[p][role] = local(part_in.at[0, 0, c, :, cols], own.at[p, role])
    state_loads = [
        local(a, b)
        for a, b in (
            (ms_in, l_ms), (vs_in, l_vs), (master_in, l_master), (mc_in, l_mc), (vc_in, l_vc),
        )
    ]

    barrier = pltpu.get_barrier_semaphore()
    xc_peers, xy_peers, zc_peers = [], [], []
    for d in range(1, 8):
        k = mod(own_k + d, 8)
        xc_peers.append((k, {"x": k // 2, "c": lax.rem(k, 2)}))
    for d in (10, 9, 11, 6, 14, 2, 8, 5, 7, 13, 15, 1, 3, 4, 12):
        xy_peers.append({"x": mod(x + d // 4, 4), "y": mod(y + d % 4, 4)})
    for d in (8, 9, 6, 7, 10, 11, 4, 5, 12, 13, 2, 3, 14, 15, 1):
        zc_peers.append({"z": mod(z + d // 2, 8), "c": lax.rem(c + d % 2, 2)})
    greeted = list(xy_peers) + list(zc_peers)
    greeted += [{"x": mod(x + d, 4), "c": other} for d in (1, 2, 3)]
    greeted += [{"y": mod(y + d, 4), "c": other} for d in (1, 3)]
    for dev in greeted:
        pl.semaphore_signal(barrier, inc=1, device_id=dev, device_id_type=MESH)
    pl.semaphore_wait(barrier, len(greeted))

    state = group()
    tile_cols = [
        lambda kx: col(kx * WIDE + y * SUB, SUB),
        lambda kx: col(HALF + y * WIDE + kx * SUB, SUB),
    ]
    own_state = []
    for src, dst in ((master_in, e_master), (mc_in, e_mc), (vc_in, e_vc)):
        for p in range(2):
            own_state.append(local(src.at[c, :, pl.ds(tile_cols[p](x), SUB)], dst.at[own_k, p]))
            for k, dev in xc_peers:
                send(src.at[dev["c"], :, pl.ds(tile_cols[p](dev["x"]), SUB)], dst.at[own_k, p], state, **dev)
    raw = [[group() for _ in range(2)] for _ in range(2)]
    for q in range(2):
        m = lax.rem(c + q, 2)
        for p in range(2):
            axis = axes[p][0]
            for h in range(2):
                cols = pl.ds(col(p * HALF + roles[p][3] * WIDE + h * (WIDE // 2), WIDE // 2), WIDE // 2)
                send(part_in.at[0, 0, m, :, cols], rcv1.at[p, h, q], raw[p][h], **{axis: roles[p][h], "c": m})
    pair = [[group() for _ in range(3)] for _ in range(2)]
    for role in range(3):
        for p in range(2):
            cols = pl.ds(col(p * HALF + roles[p][role] * WIDE, WIDE), WIDE)
            send(part_in.at[0, 0, other, :, cols], par.at[p, role], pair[p][role], c=other)

    for load in state_loads:
        load.wait()
    sc_stage[...] = jnp.zeros_like(sc_stage)
    for m in range(2):
        sc_stage[m, 0:2, 0:4] = l_ms[m]
        sc_stage[m, 2:4, 0:4] = l_vs[m]
    e_s[own_k] = sc_stage[c]
    for k, dev in xc_peers:
        send(sc_stage.at[dev["c"]], e_s.at[own_k], state, **dev)

    from_side = [[group() for _ in range(2)] for _ in range(2)]
    for p in range(2):
        axis = axes[p][0]
        for side in range(2):
            own_loads[p][side].wait()
            arrived(pair[p][side], size(par.at[p, side]))
            lo = (1 - side) * (WIDE // 2)

            @pl.loop(0, V // TILE)
            def _(t):
                rows = pl.ds(pl.multiple_of(t * TILE, TILE), TILE)
                cc = pl.ds(lo, WIDE // 2)
                snd[p, side, rows, cc] = own[p, side, rows, cc].astype(F32) + par[p, side, rows, cc].astype(F32)

            cc = pl.ds(lo, WIDE // 2)
            send(snd.at[p, side, :, cc], rcv2.at[p, side, :, cc], from_side[p][side], **{axis: roles[p][side]})

    for copy in own_state:
        copy.wait()
    arrived(state, 7 * 10)
    blocks = (x // 2, 2 + y // 2)
    for k in range(8):
        e = e_s[k]
        lane = lax.broadcasted_iota(jnp.int32, e.shape, 1)
        for p in range(2):
            scale = jnp.sum(jnp.where(lane == blocks[p], e, 0.0), axis=1, keepdims=True)
            rows = pl.ds(2 * k, 2)
            tile[0, p, rows, :] = e_mc[k, p].astype(F32) * scale[0:2]
            tile[1, p, rows, :] = e_vc[k, p].astype(F32) * scale[2:4]
            tile[2, p, rows, :] = e_master[k, p]
    my_rows = pl.ds(pl.multiple_of(z * TILE, TILE), TILE)
    z_next, z_last = {"z": mod(z + 1, 8)}, {"z": mod(z - 1, 8)}
    z_rows = lambda d: pl.ds(pl.multiple_of(mod(z + d, 8) * TILE, TILE), TILE)
    column_state = [group() for _ in range(4)]
    send(tile, st.at[:, :, my_rows, :], column_state[0], **z_next)
    send(tile, st.at[:, :, my_rows, :], column_state[0], **z_last)

    def pass_state(n):
        arrived(column_state[n - 1], 2 * 96)
        for d, dev, p in ((-n, z_next, 0), (n, z_last, 1)):
            ref = st.at[:, :, z_rows(d), :] if n < 3 else st.at[:, p, z_rows(d), :]
            send(ref, ref, column_state[n], **dev)

    for n in range(3):
        for p in range(2):
            st[n, p, my_rows, :] = tile[n, p]

    half_subs = []
    for p in range(2):
        i2 = axes[p][3]
        half_subs.append([
            tuple(2 * h + lax.rem(i2 + i2 // 2 + h + 1 - n, 2) for h in range(2)) for n in range(2)
        ])
    relay = [[[group() for _ in range(2)] for _ in range(2)] for _ in range(2)]
    for n in range(2):
        for p in range(2):
            axis = axes[p][0]
            for side in range(2):
                sub = half_subs[p][n][side]
                if n == 0:
                    arrived(raw[p][side], size(rcv1.at[p, side]))
                cc = pl.ds(col(sub * SUB, SUB), SUB)
                cr = pl.ds(col((sub - 2 * side) * SUB, SUB), SUB)

                @pl.loop(0, V // TILE)
                def _(t):
                    rows = pl.ds(pl.multiple_of(t * TILE, TILE), TILE)
                    near = own[p, side, rows, cc].astype(F32) + par[p, side, rows, cc].astype(F32)
                    far = rcv1[p, side, 0, rows, cr].astype(F32) + rcv1[p, side, 1, rows, cr].astype(F32)
                    snd[p, side, rows, cc] = near + far

                send(snd.at[p, side, :, cc], rcv2.at[p, side, :, cc], relay[p][side][n], **{axis: roles[p][side]})
    pass_state(1)

    second = [group() for _ in range(2)]
    for n in range(2):
        for p in range(2):
            axis2, i2 = axes[p][2], axes[p][3]
            if n == 0:
                own_loads[p][2].wait()
                arrived(pair[p][2], size(par.at[p, 2]))
                for side in range(2):
                    arrived(from_side[p][side], size(rcv2.at[p, side]) // 2)
            for h in range(2):
                arrived(relay[p][h][n], size(rcv2.at[p, h]) // 4)
                cols = pl.ds(col(half_subs[p][n][h] * SUB, SUB), SUB)

                @pl.loop(0, V // TILE)
                def _(t):
                    rows = pl.ds(pl.multiple_of(t * TILE, TILE), TILE)
                    near = own[p, 2, rows, cols].astype(F32) + par[p, 2, rows, cols].astype(F32)
                    s_buf[p, rows, cols] = near + rcv2[p, 0, rows, cols] + rcv2[p, 1, rows, cols]

            opp2 = roles2[p][3]
            if n == 0:
                targets = ((opp2, 0), (i2 + 1 - 2 * lax.rem(i2, 2), 1))
            else:
                targets = ((opp2 + 1 - 2 * lax.rem(opp2, 2), 2),)
            for target, slot in targets:
                cols = pl.ds(col(target * SUB, SUB), SUB)
                send(s_buf.at[p, :, cols], p2f.at[p, slot], second[p], **{axis2: target})
        pass_state(2 + n)

    third = [group() for _ in range(2)]
    for p in range(2):
        r2 = roles2[p]
        arrived(second[p], size(p2f.at[p]))
        cols = pl.ds(col(r2[2] * SUB, SUB), SUB)

        @pl.loop(0, V // TILE)
        def _(t):
            rows = pl.ds(pl.multiple_of(t * TILE, TILE), TILE)
            t_buf[p, rows, :] = s_buf[p, rows, cols] + p2f[p, 0, rows] + (p2f[p, 1, rows] + p2f[p, 2, rows])

        for d in (4, 3, 5, 2, 6, 1, 7):
            zd = mod(z + d, 8)
            rows = pl.ds(pl.multiple_of(zd * TILE, TILE), TILE)
            send(t_buf.at[p, rows, :], z_buf.at[p, d - 1], third[p], z=zd)

    square = jnp.zeros((8, 128), F32)
    for p in range(2):
        arrived(third[p], size(z_buf.at[p]))
        g = t_buf[p, my_rows, :]
        for d in range(7):
            g = g + z_buf[p, d]
        g_buf[p] = g
        g_col[p, my_rows, :] = g
        sq = g * g
        for i in range(2):
            for j in range(2):
                square = square + sq[8 * i:8 * i + 8, 128 * j:128 * j + 128]
    norm_zc, norm_xy, q1, q2, column_g = (group() for _ in range(5))
    slot = 2 * z + c
    nzc[slot] = square
    for dev in zc_peers:
        send(nzc.at[slot], nzc.at[slot], norm_zc, **dev)
    for d in (4, 3, 5, 2, 6, 1, 7):
        send(g_buf, g_col.at[:, my_rows, :], column_g, z=mod(z + d, 8))

    for p in range(2):
        for k in range(8):
            q_s[k, p] = g_buf[p, 2 * k:2 * k + 2, :]
    for k, dev in xc_peers:
        send(q_s.at[k], q_r.at[own_k], q1, **dev)
    q_r[own_k] = q_s[own_k]

    arrived(norm_zc, 15 * 4)
    slot = 4 * x + y
    nxy[slot] = functools.reduce(lambda a, b: a + b, [nzc[k] for k in range(16)])
    for dev in xy_peers:
        send(nxy.at[slot], nxy.at[slot], norm_xy, **dev)

    arrived(q1, 7 * 4)
    for d in (2, 1, 3):
        send(q_r, g_full.at[y], q2, y=mod(y + d, 4))
    g_full[y] = q_r[...]

    arrived(norm_xy, 15 * 4)
    total = functools.reduce(lambda a, b: a + b, [nxy[k] for k in range(16)])
    total = jnp.sum(jnp.sum(total, axis=1, keepdims=True), axis=0, keepdims=True)
    clip = 1.0 / jnp.maximum(jnp.sqrt(total), 1.0)

    block_of = lambda p, i, j: pl.ds(col(p * HALF + i * WIDE + j * SUB, SUB), SUB)
    to_pair = group()
    rows_half = (pl.ds(0, V // 2), pl.ds(V // 2, V // 2))
    block_kib = V * SUB * 2 // 1024

    def finished(p, i, j):
        ref = o_w.at[c, :, block_of(p, i, j)]
        send(ref, ref, to_pair, c=other)

    def spread(p, i, j, axis, targets):
        ref = o_w.at[c, :, block_of(p, i, j)]
        ks = [group() for _ in targets]
        for k, target in zip(ks, targets):
            send(ref, ref, k, **{axis: target})
        return ks

    def forward(p, i, j, axis, target, h, k):
        ref = o_w.at[c, rows_half[h], block_of(p, i, j)]
        send(ref, ref, k, **{axis: target})

    arrived(column_state[3], 96)
    arrived(column_g, 7 * 32)
    along2, along1 = [None] * 2, [[None] * 4 for _ in range(2)]
    for p in range(2):
        a1, i1, a2, i2 = axes[p]
        cols = block_of(p, i1, i2)

        @pl.loop(0, V // TILE)
        def _(t):
            rows = pl.ds(pl.multiple_of(t * TILE, TILE), TILE)
            _, _, fresh = adam(st[0, p, rows], st[1, p, rows], clip * g_col[p, rows], st[2, p, rows])
            o_w[c, rows, cols] = fresh.astype(BF16)

        right2, left2, _, opp2 = roles2[p]
        along2[p] = spread(p, i1, i2, a2, (opp2, right2, left2))
        along1[p][0] = spread(p, i1, i2, a1, roles[p][:2])
        finished(p, i1, i2)

    arrived(q2, 3 * 32)
    lane4 = lax.broadcasted_iota(jnp.int32, (2, 4), 1)
    for m in range(2):
        tops_m = jnp.zeros((2, 4), F32)
        tops_v = jnp.zeros((2, 4), F32)
        for b in range(4):
            cs = slice(b * BLOCK, (b + 1) * BLOCK)
            pieces = []
            for s in range(8):
                if b < 2:
                    px, py, p = 2 * b + s // 4, s % 4, 0
                else:
                    py, px, p = 2 * (b - 2) + s // 4, s % 4, 1
                pieces.append(g_full[py, 2 * px + m, p])
            g = jnp.concatenate(pieces, axis=1)
            moment = l_mc[m, :, cs].astype(F32) * l_ms[m, :, b:b + 1]
            second_ = l_vc[m, :, cs].astype(F32) * l_vs[m, :, b:b + 1]
            m2, v2, fresh = adam(moment, second_, clip * g, l_master[m, :, cs])
            m_top = jnp.max(jnp.abs(m2), axis=1, keepdims=True) + 1e-20
            v_top = jnp.max(jnp.abs(v2), axis=1, keepdims=True) + 1e-20
            o_master[m, :, cs] = fresh
            o_mc[m, :, cs] = (m2 / m_top).astype(BF16)
            o_vc[m, :, cs] = (v2 / v_top).astype(BF16)
            tops_m = jnp.where(lane4 == b, m_top, tops_m)
            tops_v = jnp.where(lane4 == b, v_top, tops_v)
        o_ms[m] = tops_m
        o_vs[m] = tops_v
    for n, s in ((1, 1), (2, 2), (0, 3)):
        for p in range(2):
            a1, i1, a2, i2 = axes[p]
            right2, left2, _, opp2 = roles2[p]
            origin = (opp2, left2, right2)[n]
            arrived(along2[p][n], block_kib)
            targets = roles[p][:2] if s < 3 else (roles[p][3],) + roles[p][:2]
            along1[p][s] = spread(p, i1, origin, a1, targets)
            finished(p, i1, origin)

    fwd1 = [[group() for _ in range(3)] for _ in range(2)]

    def column(p, s):
        right2, left2, _, opp2 = roles2[p]
        return (axes[p][3], left2, right2, opp2)[s]

    def pass_on(p, s):
        right1, left1, _, _ = roles[p]
        for side, origin in ((0, left1), (1, right1)):
            arrived(along1[p][s][side], block_kib)
            forward(p, origin, column(p, s), axes[p][0], roles[p][side], side, fwd1[p][s])
            finished(p, origin, column(p, s))

    for s in range(3):
        for p in range(2):
            pass_on(p, s)
    for s in range(3):
        for p in range(2):
            arrived(fwd1[p][s], block_kib)
            finished(p, roles[p][3], column(p, s))
    for n, role in ((1, 1), (2, 0), (0, 3)):
        for p in range(2):
            arrived(along1[p][3][n], block_kib)
            finished(p, roles[p][role], column(p, 3))
    arrived(to_pair, size(o_w.at[0]))
    all_sent()
    assert groups[0] <= SEMS and groups[1] <= LOCAL_SEMS, (groups, sent)


def write_out(*refs):
    sems = refs[12]
    copies = [pltpu.make_async_copy(refs[k], refs[k + 6], sems.at[k]) for k in (5, 0, 1, 2, 3, 4)]
    for copy in copies:
        copy.start()
    for copy in copies:
        copy.wait()


def body(partials, master, m_codes, v_codes, m_scales, v_scales):
    any_spec = pl.BlockSpec(memory_space=pl.ANY)
    vmem = pltpu.VMEM
    small = [pltpu.with_memory_space_constraint(a, pltpu.HBM) for a in (master, m_codes, v_codes, m_scales, v_scales)]
    results = pl.pallas_call(
        kernel,
        out_shape=(
            jax.ShapeDtypeStruct(master.shape, F32),
            jax.ShapeDtypeStruct(master.shape, BF16),
            jax.ShapeDtypeStruct(master.shape, BF16),
            jax.ShapeDtypeStruct(m_scales.shape, F32),
            jax.ShapeDtypeStruct(m_scales.shape, F32),
            jax.ShapeDtypeStruct((2, V, D), BF16),
        ),
        in_specs=[pl.BlockSpec(memory_space=pltpu.HBM)] * 6,
        out_specs=(pl.BlockSpec(memory_space=pltpu.VMEM),) * 6,
        scratch_shapes=[
            vmem((2, 3, V, WIDE), BF16),
            vmem((2, 3, V, WIDE), BF16),
            vmem((2, 2, 2, V, WIDE // 2), BF16),
            vmem((2, 2, V, WIDE), F32),
            vmem((2, 2, V, WIDE), F32),
            vmem((2, V, WIDE), F32),
            vmem((2, 3, V, SUB), F32),
            vmem((2, V, SUB), F32),
            vmem((2, 7, TILE, SUB), F32),
            vmem((2, TILE, SUB), F32),
            vmem((16, 8, 128), F32),
            vmem((16, 8, 128), F32),
            vmem((8, 2, 2, SUB), F32),
            vmem((8, 2, 2, SUB), BF16),
            vmem((8, 2, 2, SUB), BF16),
            vmem((8, 4, 128), F32),
            vmem((2, 4, 128), F32),
            vmem((3, 2, TILE, SUB), F32),
            vmem((3, 2, V, SUB), F32),
            vmem((2, V, SUB), F32),
            vmem((8, 2, 2, SUB), F32),
            vmem((8, 2, 2, SUB), F32),
            vmem((4, 8, 2, 2, SUB), F32),
            vmem((2, 2, D), F32),
            vmem((2, 2, D), BF16),
            vmem((2, 2, D), BF16),
            vmem((2, 2, 4), F32),
            vmem((2, 2, 4), F32),
            vmem((LIMIT_KIB, 2, 128), F32),
            pltpu.SemaphoreType.DMA((1,)),
            pltpu.SemaphoreType.DMA((SEMS,)),
            pltpu.SemaphoreType.DMA((LOCAL_SEMS,)),
        ],
        compiler_params=pltpu.CompilerParams(
            collective_id=0, has_side_effects=True, vmem_limit_bytes=48 * 1024 * 1024
        ),
        name="step",
    )(partials, *small)
    return pl.pallas_call(
        write_out,
        out_shape=tuple(jax.ShapeDtypeStruct(a.shape, a.dtype) for a in results),
        in_specs=[any_spec] * 6,
        out_specs=(any_spec,) * 6,
        scratch_shapes=[pltpu.SemaphoreType.DMA((6,))],
        compiler_params=pltpu.CompilerParams(vmem_limit_bytes=1024 * 1024),
        name="write_out",
    )(*results)


def solution(mesh):
    finer = Mesh(mesh.devices.reshape(NZ, NX, NC, NY), ("z", "x", "c", "y"))
    rows = P(None, ("z", "x", "c"), None)
    return jax.shard_map(
        body,
        mesh=finer,
        in_specs=(P("y", ("z", "x", "c"), None, None, None),) + (rows,) * 5,
        out_specs=(rows,) * 5 + (P(),),
        check_vma=False,
    )
```

```python
import functools
import math

import jax
import jax.numpy as jnp
from jax import lax
from jax.experimental import pallas as pl
from jax.experimental.pallas import tpu as pltpu
from jax.sharding import Mesh
from jax.sharding import PartitionSpec as P

BLOCK = 2048
STEP = 10
MESH = pl.DeviceIdType.MESH
F32 = jnp.float32
BF16 = jnp.bfloat16

V = 128
D = 8192
HALF = 4096
WIDE = 1024
SUB = 256
NX, NY, NZ, NC = 4, 4, 8, 2
TILE = 16
SEMS = 80
LOCAL_SEMS = 18
LIMIT_KIB = 12 * 1024


def mod(a, n):
    return lax.rem(a + n, n)


def col(value, step):
    return pl.multiple_of(value, step)


def adam(moment, second, scaled, master):
    m2 = 0.9 * moment + 0.1 * scaled
    v2 = 0.95 * second + 0.05 * scaled * scaled
    update = m2 / (1.0 - 0.9**STEP) / (jnp.sqrt(v2 / (1.0 - 0.95**STEP)) + 1e-08)
    return m2, v2, master - 0.01 * update


def kernel(
    part_in, master_in, mc_in, vc_in, ms_in, vs_in,
    o_master, o_mc, o_vc, o_ms, o_vs, o_w,
    own, par, rcv1, snd, rcv2, s_buf, p2f, t_buf, z_buf, g_buf,
    nzc, nxy,
    e_master, e_mc, e_vc, e_s, sc_stage, tile, st, g_col,
    q_s, q_r, g_full,
    l_master, l_mc, l_vc, l_ms, l_vs, bytes_ref,
    ssem, rsem, lsem,
):
    x, y, z, c = (lax.axis_index(a) for a in ("x", "y", "z", "c"))
    other = 1 - c
    groups, sent = [0, 0], [0]

    def size(ref):
        return math.prod(ref.shape) * ref.dtype.itemsize / 1024

    def group():
        groups[0] += 1
        return groups[0] - 1

    def send(src, dst, k, **dev):
        sent[0] += size(src)
        pltpu.make_async_remote_copy(
            src_ref=src, dst_ref=dst, send_sem=ssem.at[0], recv_sem=rsem.at[k],
            device_id=dev, device_id_type=MESH,
        ).start()

    def arrived(k, kib):
        ref = bytes_ref.at[pl.ds(0, int(2 * kib))]
        pltpu.make_async_copy(ref, ref, rsem.at[k]).wait()

    def arrived_words(k, slots):
        arrived(k, 15 * size(slots.at[0]))

    def all_sent():
        assert sent[0] <= LIMIT_KIB
        ref = bytes_ref.at[pl.ds(0, int(2 * sent[0]))]
        pltpu.make_async_copy(ref, ref, ssem.at[0]).wait()


    def local(src, dst):
        groups[1] += 1
        copy = pltpu.make_async_copy(src, dst, lsem.at[groups[1] - 1])
        copy.start()
        return copy


    axes = (("x", x, "y", y), ("y", y, "x", x))
    roles = [tuple(mod(i + d, 4) for d in (1, -1, 0, 2)) for _, i, _, _ in axes]
    roles2 = [tuple(mod(j + d, 4) for d in (1, -1, 0, 2)) for _, _, _, j in axes]
    own_k = 2 * x + c

    own_loads = [[None] * 3 for _ in range(2)]
    for role in range(3):
        for p in range(2):
            cols = pl.ds(col(p * HALF + roles[p][role] * WIDE, WIDE), WIDE)
            own_loads[p][role] = local(part_in.at[0, 0, c, :, cols], own.at[p, role])
    state_loads = [
        local(a, b)
        for a, b in (
            (ms_in, l_ms), (vs_in, l_vs), (master_in, l_master), (mc_in, l_mc), (vc_in, l_vc),
        )
    ]

    barrier = pltpu.get_barrier_semaphore()
    xc_peers, xy_peers, zc_peers = [], [], []
    for d in range(1, 8):
        k = mod(own_k + d, 8)
        xc_peers.append((k, {"x": k // 2, "c": lax.rem(k, 2)}))
    for d in (10, 9, 11, 6, 14, 2, 8, 5, 7, 13, 15, 1, 3, 4, 12):
        xy_peers.append({"x": mod(x + d // 4, 4), "y": mod(y + d % 4, 4)})
    for d in (8, 9, 6, 7, 10, 11, 4, 5, 12, 13, 2, 3, 14, 15, 1):
        zc_peers.append({"z": mod(z + d // 2, 8), "c": lax.rem(c + d % 2, 2)})
    greeted = list(xy_peers) + list(zc_peers)
    greeted += [{"x": mod(x + d, 4), "c": other} for d in (1, 2, 3)]
    greeted += [{"y": mod(y + d, 4), "c": other} for d in (1, 3)]
    for dev in greeted:
        pl.semaphore_signal(barrier, inc=1, device_id=dev, device_id_type=MESH)
    pl.semaphore_wait(barrier, len(greeted))

    raw = [[group() for _ in range(2)] for _ in range(2)]
    for q in range(2):
        m = lax.rem(c + q, 2)
        for p in range(2):
            axis = axes[p][0]
            for h in range(2):
                cols = pl.ds(col(p * HALF + roles[p][3] * WIDE + h * (WIDE // 2), WIDE // 2), WIDE // 2)
                send(part_in.at[0, 0, m, :, cols], rcv1.at[p, h, q], raw[p][h], **{axis: roles[p][h], "c": m})
    pair = [[group() for _ in range(3)] for _ in range(2)]
    for role in range(3):
        for p in range(2):
            cols = pl.ds(col(p * HALF + roles[p][role] * WIDE, WIDE), WIDE)
            send(part_in.at[0, 0, other, :, cols], par.at[p, role], pair[p][role], c=other)

    state = group()
    tile_cols = [
        lambda kx: col(kx * WIDE + y * SUB, SUB),
        lambda kx: col(HALF + y * WIDE + kx * SUB, SUB),
    ]
    own_state = []
    for src, dst in ((master_in, e_master), (mc_in, e_mc), (vc_in, e_vc)):
        for p in range(2):
            own_state.append(local(src.at[c, :, pl.ds(tile_cols[p](x), SUB)], dst.at[own_k, p]))
            for k, dev in xc_peers:
                send(src.at[dev["c"], :, pl.ds(tile_cols[p](dev["x"]), SUB)], dst.at[own_k, p], state, **dev)
    for load in state_loads:
        load.wait()
    sc_stage[...] = jnp.zeros_like(sc_stage)
    for m in range(2):
        sc_stage[m, 0:2, 0:4] = l_ms[m]
        sc_stage[m, 2:4, 0:4] = l_vs[m]
    e_s[own_k] = sc_stage[c]
    for k, dev in xc_peers:
        send(sc_stage.at[dev["c"]], e_s.at[own_k], state, **dev)

    from_side = [[group() for _ in range(2)] for _ in range(2)]
    for p in range(2):
        axis = axes[p][0]
        for side in range(2):
            own_loads[p][side].wait()
            arrived(pair[p][side], size(par.at[p, side]))
            lo = (1 - side) * (WIDE // 2)

            @pl.loop(0, V // TILE)
            def _(t):
                rows = pl.ds(pl.multiple_of(t * TILE, TILE), TILE)
                cc = pl.ds(lo, WIDE // 2)
                snd[p, side, rows, cc] = own[p, side, rows, cc].astype(F32) + par[p, side, rows, cc].astype(F32)

            cc = pl.ds(lo, WIDE // 2)
            send(snd.at[p, side, :, cc], rcv2.at[p, side, :, cc], from_side[p][side], **{axis: roles[p][side]})

    for copy in own_state:
        copy.wait()
    arrived(state, 7 * 10)
    blocks = (x // 2, 2 + y // 2)
    for k in range(8):
        e = e_s[k]
        lane = lax.broadcasted_iota(jnp.int32, e.shape, 1)
        for p in range(2):
            scale = jnp.sum(jnp.where(lane == blocks[p], e, 0.0), axis=1, keepdims=True)
            rows = pl.ds(2 * k, 2)
            tile[0, p, rows, :] = e_mc[k, p].astype(F32) * scale[0:2]
            tile[1, p, rows, :] = e_vc[k, p].astype(F32) * scale[2:4]
            tile[2, p, rows, :] = e_master[k, p]
    my_rows = pl.ds(pl.multiple_of(z * TILE, TILE), TILE)
    z_next, z_last = {"z": mod(z + 1, 8)}, {"z": mod(z - 1, 8)}
    z_rows = lambda d: pl.ds(pl.multiple_of(mod(z + d, 8) * TILE, TILE), TILE)
    column_state = [group() for _ in range(4)]
    send(tile, st.at[:, :, my_rows, :], column_state[0], **z_next)
    send(tile, st.at[:, :, my_rows, :], column_state[0], **z_last)

    def pass_state(n):
        arrived(column_state[n - 1], 2 * 96)
        for d, dev, p in ((-n, z_next, 0), (n, z_last, 1)):
            ref = st.at[:, :, z_rows(d), :] if n < 3 else st.at[:, p, z_rows(d), :]
            send(ref, ref, column_state[n], **dev)

    for n in range(3):
        for p in range(2):
            st[n, p, my_rows, :] = tile[n, p]

    half_subs = []
    for p in range(2):
        i2 = axes[p][3]
        half_subs.append([
            tuple(2 * h + lax.rem(i2 + i2 // 2 + h + 1 - min(n, 1), 2) for h in range(2)) for n in range(3)
        ])
    starts, widths = (0, 0, SUB // 2), (SUB, SUB // 2, SUB // 2)
    relay = [[[group() for _ in range(3)] for _ in range(2)] for _ in range(2)]
    for n in range(3):
        for p in range(2):
            axis = axes[p][0]
            for side in range(2):
                sub = half_subs[p][n][side]
                if n == 0:
                    arrived(raw[p][side], size(rcv1.at[p, side]))
                cc = pl.ds(col(sub * SUB + starts[n], SUB // 2), widths[n])
                cr = pl.ds(col((sub - 2 * side) * SUB + starts[n], SUB // 2), widths[n])

                @pl.loop(0, V // TILE)
                def _(t):
                    rows = pl.ds(pl.multiple_of(t * TILE, TILE), TILE)
                    near = own[p, side, rows, cc].astype(F32) + par[p, side, rows, cc].astype(F32)
                    far = rcv1[p, side, 0, rows, cr].astype(F32) + rcv1[p, side, 1, rows, cr].astype(F32)
                    snd[p, side, rows, cc] = near + far

                send(snd.at[p, side, :, cc], rcv2.at[p, side, :, cc], relay[p][side][n], **{axis: roles[p][side]})
    pass_state(1)

    second = [[group() for _ in range(3)] for _ in range(2)]
    for n in range(3):
        for p in range(2):
            axis2, i2 = axes[p][2], axes[p][3]
            if n == 0:
                own_loads[p][2].wait()
                arrived(pair[p][2], size(par.at[p, 2]))
                for side in range(2):
                    arrived(from_side[p][side], size(rcv2.at[p, side]) // 2)
            for h in range(2):
                arrived(relay[p][h][n], V * widths[n] * 4 / 1024)
                cols = pl.ds(col(half_subs[p][n][h] * SUB + starts[n], SUB // 2), widths[n])

                @pl.loop(0, V // TILE)
                def _(t):
                    rows = pl.ds(pl.multiple_of(t * TILE, TILE), TILE)
                    near = own[p, 2, rows, cols].astype(F32) + par[p, 2, rows, cols].astype(F32)
                    s_buf[p, rows, cols] = near + rcv2[p, 0, rows, cols] + rcv2[p, 1, rows, cols]

            opp2 = roles2[p][3]
            if n == 0:
                targets = ((opp2, 0), (i2 + 1 - 2 * lax.rem(i2, 2), 1))
            else:
                targets = ((opp2 + 1 - 2 * lax.rem(opp2, 2), 2),)
            for target, slot in targets:
                cols = pl.ds(col(target * SUB + starts[n], SUB // 2), widths[n])
                send(s_buf.at[p, :, cols], p2f.at[p, slot, :, starts[n]:starts[n] + widths[n]], second[p][n],
                     **{axis2: target})
        if n < 2:
            pass_state(2 + n)

    third = [[group() for _ in range(2)] for _ in range(2)]
    for q in range(2):
        for p in range(2):
            i2 = axes[p][3]
            if q == 0:
                arrived(second[p][0], 2 * V * SUB * 4 / 1024)
            arrived(second[p][1 + q], V * SUB * 2 / 1024)
            cols = pl.ds(col(i2 * SUB + q * (SUB // 2), SUB // 2), SUB // 2)
            cq = pl.ds(q * (SUB // 2), SUB // 2)

            @pl.loop(0, V // TILE)
            def _(t):
                rows = pl.ds(pl.multiple_of(t * TILE, TILE), TILE)
                t_buf[p, q, rows, :] = s_buf[p, rows, cols] + p2f[p, 0, rows, cq] + (
                    p2f[p, 1, rows, cq] + p2f[p, 2, rows, cq])

            for d in (4, 3, 5, 2, 6, 1, 7):
                zd = mod(z + d, 8)
                rows = pl.ds(pl.multiple_of(zd * TILE, TILE), TILE)
                send(t_buf.at[p, q, rows, :], z_buf.at[p, q, d - 1], third[p][q], z=zd)

    square = jnp.zeros((8, 128), F32)
    for q in range(2):
        for p in range(2):
            arrived(third[p][q], size(z_buf.at[p, q]))
            g = t_buf[p, q, my_rows, :]
            for d in range(7):
                g = g + z_buf[p, q, d]
            cq = slice(q * (SUB // 2), (q + 1) * (SUB // 2))
            g_buf[p, :, cq] = g
            g_col[p, my_rows, cq] = g
            sq = g * g
            square = square + sq[0:8] + sq[8:16]
    norm_zc, norm_xy, q1, q2, column_g = (group() for _ in range(5))
    slot = 2 * z + c
    nzc[slot] = jnp.sum(square, axis=0, keepdims=True)
    for dev in zc_peers:
        send(nzc.at[slot], nzc.at[slot], norm_zc, **dev)
    for d in (4, 3, 5, 2, 6, 1, 7):
        send(g_buf, g_col.at[:, my_rows, :], column_g, z=mod(z + d, 8))

    for p in range(2):
        for k in range(8):
            q_s[k, p] = g_buf[p, 2 * k:2 * k + 2, :]
    for k, dev in xc_peers:
        send(q_s.at[k], q_r.at[own_k], q1, **dev)
    q_r[own_k] = q_s[own_k]

    arrived_words(norm_zc, nzc)
    slot = 4 * x + y
    nxy[slot] = functools.reduce(lambda a, b: a + b, [nzc[k] for k in range(16)])
    for dev in xy_peers:
        send(nxy.at[slot], nxy.at[slot], norm_xy, **dev)

    arrived(q1, 7 * 4)
    for d in (2, 1, 3):
        send(q_r, g_full.at[y], q2, y=mod(y + d, 4))
    g_full[y] = q_r[...]

    arrived_words(norm_xy, nxy)
    total = functools.reduce(lambda a, b: a + b, [nxy[k] for k in range(16)])
    total = jnp.sum(total, axis=1, keepdims=True)
    clip = 1.0 / jnp.maximum(jnp.sqrt(total), 1.0)

    block_of = lambda p, i, j: pl.ds(col(p * HALF + i * WIDE + j * SUB, SUB), SUB)
    to_pair = group()
    rows_half = (pl.ds(0, V // 2), pl.ds(V // 2, V // 2))
    block_kib = V * SUB * 2 // 1024

    def finished(p, i, j):
        ref = o_w.at[c, :, block_of(p, i, j)]
        send(ref, ref, to_pair, c=other)

    def spread(p, i, j, axis, targets):
        ref = o_w.at[c, :, block_of(p, i, j)]
        ks = [group() for _ in targets]
        for k, target in zip(ks, targets):
            send(ref, ref, k, **{axis: target})
        return ks

    def forward(p, i, j, axis, target, h, k):
        ref = o_w.at[c, rows_half[h], block_of(p, i, j)]
        send(ref, ref, k, **{axis: target})

    arrived(column_state[3], 96)
    arrived(column_g, 7 * 32)
    along2, along1 = [None] * 2, [[None] * 4 for _ in range(2)]
    for p in range(2):
        a1, i1, a2, i2 = axes[p]
        cols = block_of(p, i1, i2)

        @pl.loop(0, V // TILE)
        def _(t):
            rows = pl.ds(pl.multiple_of(t * TILE, TILE), TILE)
            _, _, fresh = adam(st[0, p, rows], st[1, p, rows], clip * g_col[p, rows], st[2, p, rows])
            o_w[c, rows, cols] = fresh.astype(BF16)

        right2, left2, _, opp2 = roles2[p]
        along2[p] = spread(p, i1, i2, a2, (right2, left2, opp2))
        along1[p][0] = spread(p, i1, i2, a1, roles[p][:2])
        finished(p, i1, i2)

    for n, s in ((1, 1), (0, 2), (2, 3)):
        for p in range(2):
            a1, i1, a2, i2 = axes[p]
            right2, left2, _, opp2 = roles2[p]
            origin = (left2, right2, opp2)[n]
            arrived(along2[p][n], block_kib)
            along1[p][s] = spread(p, i1, origin, a1, roles[p][:2])
            finished(p, i1, origin)

    fwd1 = [[group() for _ in range(4)] for _ in range(2)]

    def column(p, s):
        right2, left2, _, opp2 = roles2[p]
        return (axes[p][3], right2, left2, opp2)[s]

    def pass_on(p, s):
        right1, left1, _, _ = roles[p]
        for side, origin in ((0, left1), (1, right1)):
            arrived(along1[p][s][side], block_kib)
            forward(p, origin, column(p, s), axes[p][0], roles[p][side], side, fwd1[p][s])
            finished(p, origin, column(p, s))

    arrived(q2, 3 * 32)
    lane4 = lax.broadcasted_iota(jnp.int32, (2, 4), 1)
    for m in range(2):
        tops_m = jnp.zeros((2, 4), F32)
        tops_v = jnp.zeros((2, 4), F32)
        for b in range(4):
            cs = slice(b * BLOCK, (b + 1) * BLOCK)
            pieces = []
            for s in range(8):
                if b < 2:
                    px, py, p = 2 * b + s // 4, s % 4, 0
                else:
                    py, px, p = 2 * (b - 2) + s // 4, s % 4, 1
                pieces.append(g_full[py, 2 * px + m, p])
            g = jnp.concatenate(pieces, axis=1)
            moment = l_mc[m, :, cs].astype(F32) * l_ms[m, :, b:b + 1]
            second_ = l_vc[m, :, cs].astype(F32) * l_vs[m, :, b:b + 1]
            m2, v2, fresh = adam(moment, second_, clip * g, l_master[m, :, cs])
            m_top = jnp.max(jnp.abs(m2), axis=1, keepdims=True) + 1e-20
            v_top = jnp.max(jnp.abs(v2), axis=1, keepdims=True) + 1e-20
            o_master[m, :, cs] = fresh
            o_mc[m, :, cs] = (m2 / m_top).astype(BF16)
            o_vc[m, :, cs] = (v2 / v_top).astype(BF16)
            tops_m = jnp.where(lane4 == b, m_top, tops_m)
            tops_v = jnp.where(lane4 == b, v_top, tops_v)
        o_ms[m] = tops_m
        o_vs[m] = tops_v
    for s in range(4):
        for p in range(2):
            pass_on(p, s)
    for s in range(4):
        for p in range(2):
            arrived(fwd1[p][s], block_kib)
            finished(p, roles[p][3], column(p, s))
    arrived(to_pair, size(o_w.at[0]))
    all_sent()
    assert groups[0] <= SEMS and groups[1] <= LOCAL_SEMS, (groups, sent)


def write_out(*refs):
    sems = refs[12]
    copies = [pltpu.make_async_copy(refs[k], refs[k + 6], sems.at[k]) for k in (5, 0, 1, 2, 3, 4)]
    for copy in copies:
        copy.start()
    for copy in copies:
        copy.wait()


def body(partials, master, m_codes, v_codes, m_scales, v_scales):
    any_spec = pl.BlockSpec(memory_space=pl.ANY)
    vmem = pltpu.VMEM
    small = [pltpu.with_memory_space_constraint(a, pltpu.HBM) for a in (master, m_codes, v_codes, m_scales, v_scales)]
    results = pl.pallas_call(
        kernel,
        out_shape=(
            jax.ShapeDtypeStruct(master.shape, F32),
            jax.ShapeDtypeStruct(master.shape, BF16),
            jax.ShapeDtypeStruct(master.shape, BF16),
            jax.ShapeDtypeStruct(m_scales.shape, F32),
            jax.ShapeDtypeStruct(m_scales.shape, F32),
            jax.ShapeDtypeStruct((2, V, D), BF16),
        ),
        in_specs=[pl.BlockSpec(memory_space=pltpu.HBM)] * 6,
        out_specs=(pl.BlockSpec(memory_space=pltpu.VMEM),) * 6,
        scratch_shapes=[
            vmem((2, 3, V, WIDE), BF16),
            vmem((2, 3, V, WIDE), BF16),
            vmem((2, 2, 2, V, WIDE // 2), BF16),
            vmem((2, 2, V, WIDE), F32),
            vmem((2, 2, V, WIDE), F32),
            vmem((2, V, WIDE), F32),
            vmem((2, 3, V, SUB), F32),
            vmem((2, 2, V, SUB // 2), F32),
            vmem((2, 2, 7, TILE, SUB // 2), F32),
            vmem((2, TILE, SUB), F32),
            vmem((16, 1, 128), F32),
            vmem((16, 1, 128), F32),
            vmem((8, 2, 2, SUB), F32),
            vmem((8, 2, 2, SUB), BF16),
            vmem((8, 2, 2, SUB), BF16),
            vmem((8, 4, 128), F32),
            vmem((2, 4, 128), F32),
            vmem((3, 2, TILE, SUB), F32),
            vmem((3, 2, V, SUB), F32),
            vmem((2, V, SUB), F32),
            vmem((8, 2, 2, SUB), F32),
            vmem((8, 2, 2, SUB), F32),
            vmem((4, 8, 2, 2, SUB), F32),
            vmem((2, 2, D), F32),
            vmem((2, 2, D), BF16),
            vmem((2, 2, D), BF16),
            vmem((2, 2, 4), F32),
            vmem((2, 2, 4), F32),
            vmem((2 * LIMIT_KIB, 1, 128), F32),
            pltpu.SemaphoreType.DMA((1,)),
            pltpu.SemaphoreType.DMA((SEMS,)),
            pltpu.SemaphoreType.DMA((LOCAL_SEMS,)),
        ],
        compiler_params=pltpu.CompilerParams(
            collective_id=0, has_side_effects=True, vmem_limit_bytes=48 * 1024 * 1024
        ),
        name="step",
    )(partials, *small)
    return pl.pallas_call(
        write_out,
        out_shape=tuple(jax.ShapeDtypeStruct(a.shape, a.dtype) for a in results),
        in_specs=[any_spec] * 6,
        out_specs=(any_spec,) * 6,
        scratch_shapes=[pltpu.SemaphoreType.DMA((6,))],
        compiler_params=pltpu.CompilerParams(vmem_limit_bytes=1024 * 1024),
        name="write_out",
    )(*results)


def solution(mesh):
    finer = Mesh(mesh.devices.reshape(NZ, NX, NC, NY), ("z", "x", "c", "y"))
    rows = P(None, ("z", "x", "c"), None)
    return jax.shard_map(
        body,
        mesh=finer,
        in_specs=(P("y", ("z", "x", "c"), None, None, None),) + (rows,) * 5,
        out_specs=(rows,) * 5 + (P(),),
        check_vma=False,
    )
```

```python
import functools
import math

import jax
import jax.numpy as jnp
from jax import lax
from jax.experimental import pallas as pl
from jax.experimental.pallas import tpu as pltpu
from jax.sharding import Mesh
from jax.sharding import PartitionSpec as P

BLOCK = 2048
STEP = 10
MESH = pl.DeviceIdType.MESH
F32 = jnp.float32
BF16 = jnp.bfloat16

V = 128
D = 8192
HALF = 4096
WIDE = 1024
SUB = 256
NX, NY, NZ, NC = 4, 4, 8, 2
TILE = 16
SEMS = 81
LOCAL_SEMS = 17
DIRECT = (3,)
LIMIT_KIB = 12 * 1024


def mod(a, n):
    return lax.rem(a + n, n)


def col(value, step):
    return pl.multiple_of(value, step)


def adam(moment, second, scaled, master):
    m2 = 0.9 * moment + 0.1 * scaled
    v2 = 0.95 * second + 0.05 * scaled * scaled
    root = jnp.sqrt(v2 * (1.0 / (1.0 - 0.95**STEP))) + 1e-08
    return m2, v2, master - m2 * (0.01 / (1.0 - 0.9**STEP)) / root


def kernel(
    part_in, master_in, mc_in, vc_in, ms_in, vs_in,
    o_master, o_mc, o_vc, o_ms, o_vs, o_w,
    own, par, rcv1, snd, rcv2, s_buf, p2f, t_buf, z_buf, g_buf,
    nzc, nxy,
    e_master, e_mc, e_vc, e_s, sc_stage, tile, st, g_col,
    q_s, q_r, g_full,
    l_master, l_mc, l_vc, l_ms, l_vs, bytes_ref,
    ssem, rsem, lsem,
):
    x, y, z, c = (lax.axis_index(a) for a in ("x", "y", "z", "c"))
    other = 1 - c
    groups, sent = [0, 0], [0]

    def size(ref):
        return math.prod(ref.shape) * ref.dtype.itemsize / 1024

    def group():
        groups[0] += 1
        return groups[0] - 1

    def send(src, dst, k, **dev):
        sent[0] += size(src)
        pltpu.make_async_remote_copy(
            src_ref=src, dst_ref=dst, send_sem=ssem.at[0], recv_sem=rsem.at[k],
            device_id=dev, device_id_type=MESH,
        ).start()

    def arrived(k, kib):
        ref = bytes_ref.at[pl.ds(0, int(2 * kib))]
        pltpu.make_async_copy(ref, ref, rsem.at[k]).wait()

    def arrived_words(k, slots):
        arrived(k, 15 * size(slots.at[0]))

    def all_sent():
        assert sent[0] <= LIMIT_KIB
        ref = bytes_ref.at[pl.ds(0, int(2 * sent[0]))]
        pltpu.make_async_copy(ref, ref, ssem.at[0]).wait()


    def local(src, dst):
        groups[1] += 1
        copy = pltpu.make_async_copy(src, dst, lsem.at[groups[1] - 1])
        copy.start()
        return copy


    axes = (("x", x, "y", y), ("y", y, "x", x))
    roles = [tuple(mod(i + d, 4) for d in (1, -1, 0, 2)) for _, i, _, _ in axes]
    roles2 = [tuple(mod(j + d, 4) for d in (1, -1, 0, 2)) for _, _, _, j in axes]
    own_k = 2 * x + c

    own_loads = [[None] * 3 for _ in range(2)]
    for role in range(3):
        for p in range(2):
            cols = pl.ds(col(p * HALF + roles[p][role] * WIDE, WIDE), WIDE)
            own_loads[p][role] = local(part_in.at[0, 0, c, :, cols], own.at[p, role])
    state_loads = [
        local(a, b)
        for a, b in (
            (ms_in, l_ms), (vs_in, l_vs), (master_in, l_master), (mc_in, l_mc), (vc_in, l_vc),
        )
    ]

    barrier = pltpu.get_barrier_semaphore()
    xc_peers, xy_peers, zc_peers = [], [], []
    for d in range(1, 8):
        k = mod(own_k + d, 8)
        xc_peers.append((k, {"x": k // 2, "c": lax.rem(k, 2)}))
    for d in (10, 9, 11, 6, 14, 2, 8, 5, 7, 13, 15, 1, 3, 4, 12):
        xy_peers.append({"x": mod(x + d // 4, 4), "y": mod(y + d % 4, 4)})
    for d in (8, 9, 6, 7, 10, 11, 4, 5, 12, 13, 2, 3, 14, 15, 1):
        zc_peers.append({"z": mod(z + d // 2, 8), "c": lax.rem(c + d % 2, 2)})
    greeted = list(xy_peers) + list(zc_peers)
    greeted += [{"x": mod(x + d, 4), "c": other} for d in (1, 2, 3)]
    greeted += [{"y": mod(y + d, 4), "c": other} for d in (1, 3)]
    for dev in greeted:
        pl.semaphore_signal(barrier, inc=1, device_id=dev, device_id_type=MESH)
    pl.semaphore_wait(barrier, len(greeted))

    raw = [[group() for _ in range(2)] for _ in range(2)]
    for q in range(2):
        m = lax.rem(c + q, 2)
        for p in range(2):
            axis = axes[p][0]
            for h in range(2):
                cols = pl.ds(col(p * HALF + roles[p][3] * WIDE + h * (WIDE // 2), WIDE // 2), WIDE // 2)
                send(part_in.at[0, 0, m, :, cols], rcv1.at[p, h, q], raw[p][h], **{axis: roles[p][h], "c": m})
    pair = [[group() for _ in range(3)] for _ in range(2)]
    for role in range(3):
        for p in range(2):
            cols = pl.ds(col(p * HALF + roles[p][role] * WIDE, WIDE), WIDE)
            send(part_in.at[0, 0, other, :, cols], par.at[p, role], pair[p][role], c=other)

    state = group()
    tile_cols = [
        lambda kx: col(kx * WIDE + y * SUB, SUB),
        lambda kx: col(HALF + y * WIDE + kx * SUB, SUB),
    ]
    own_state = []
    for src, dst in ((master_in, e_master), (mc_in, e_mc), (vc_in, e_vc)):
        for p in range(2):
            own_state.append(local(src.at[c, :, pl.ds(tile_cols[p](x), SUB)], dst.at[own_k, p]))
            for k, dev in xc_peers:
                send(src.at[dev["c"], :, pl.ds(tile_cols[p](dev["x"]), SUB)], dst.at[own_k, p], state, **dev)
    for load in state_loads:
        load.wait()
    sc_stage[...] = jnp.zeros_like(sc_stage)
    for m in range(2):
        sc_stage[m, 0:2, 0:4] = l_ms[m]
        sc_stage[m, 2:4, 0:4] = l_vs[m]
    e_s[own_k] = sc_stage[c]
    for k, dev in xc_peers:
        send(sc_stage.at[dev["c"]], e_s.at[own_k], state, **dev)

    from_side = [[group() for _ in range(2)] for _ in range(2)]
    for p in range(2):
        axis = axes[p][0]
        for side in range(2):
            own_loads[p][side].wait()
            arrived(pair[p][side], size(par.at[p, side]))
            lo = (1 - side) * (WIDE // 2)

            @pl.loop(0, V // TILE)
            def _(t):
                rows = pl.ds(pl.multiple_of(t * TILE, TILE), TILE)
                cc = pl.ds(lo, WIDE // 2)
                snd[p, side, rows, cc] = own[p, side, rows, cc].astype(F32) + par[p, side, rows, cc].astype(F32)

            cc = pl.ds(lo, WIDE // 2)
            send(snd.at[p, side, :, cc], rcv2.at[p, side, :, cc], from_side[p][side], **{axis: roles[p][side]})

    for copy in own_state:
        copy.wait()
    arrived(state, 7 * 10)
    blocks = (x // 2, 2 + y // 2)
    for k in range(8):
        e = e_s[k]
        lane = lax.broadcasted_iota(jnp.int32, e.shape, 1)
        for p in range(2):
            scale = jnp.sum(jnp.where(lane == blocks[p], e, 0.0), axis=1, keepdims=True)
            rows = pl.ds(2 * k, 2)
            tile[0, p, rows, :] = e_mc[k, p].astype(F32) * scale[0:2]
            tile[1, p, rows, :] = e_vc[k, p].astype(F32) * scale[2:4]
            tile[2, p, rows, :] = e_master[k, p]
    my_rows = pl.ds(pl.multiple_of(z * TILE, TILE), TILE)
    z_next, z_last = {"z": mod(z + 1, 8)}, {"z": mod(z - 1, 8)}
    z_rows = lambda d: pl.ds(pl.multiple_of(mod(z + d, 8) * TILE, TILE), TILE)
    column_state = [group() for _ in range(4)]
    send(tile, st.at[:, :, my_rows, :], column_state[0], **z_next)
    send(tile, st.at[:, :, my_rows, :], column_state[0], **z_last)

    def pass_state(n):
        arrived(column_state[n - 1], 2 * 96)
        for d, dev, p in ((-n, z_next, 0), (n, z_last, 1)):
            ref = st.at[:, :, z_rows(d), :] if n < 3 else st.at[:, p, z_rows(d), :]
            send(ref, ref, column_state[n], **dev)

    for n in range(3):
        for p in range(2):
            st[n, p, my_rows, :] = tile[n, p]

    half_subs = []
    for p in range(2):
        i2 = axes[p][3]
        half_subs.append([
            tuple(2 * h + lax.rem(i2 + i2 // 2 + h + 1 - min(n, 1), 2) for h in range(2)) for n in range(3)
        ])
    starts, widths = (0, 0, SUB // 2), (SUB, SUB // 2, SUB // 2)
    relay = [[[group() for _ in range(3)] for _ in range(2)] for _ in range(2)]
    for n in range(3):
        for p in range(2):
            axis = axes[p][0]
            for side in range(2):
                sub = half_subs[p][n][side]
                if n == 0:
                    arrived(raw[p][side], size(rcv1.at[p, side]))
                cc = pl.ds(col(sub * SUB + starts[n], SUB // 2), widths[n])
                cr = pl.ds(col((sub - 2 * side) * SUB + starts[n], SUB // 2), widths[n])

                @pl.loop(0, V // TILE)
                def _(t):
                    rows = pl.ds(pl.multiple_of(t * TILE, TILE), TILE)
                    near = own[p, side, rows, cc].astype(F32) + par[p, side, rows, cc].astype(F32)
                    far = rcv1[p, side, 0, rows, cr].astype(F32) + rcv1[p, side, 1, rows, cr].astype(F32)
                    snd[p, side, rows, cc] = near + far

                send(snd.at[p, side, :, cc], rcv2.at[p, side, :, cc], relay[p][side][n], **{axis: roles[p][side]})
    pass_state(1)

    second = [[group() for _ in range(3)] for _ in range(2)]
    for n in range(3):
        for p in range(2):
            axis2, i2 = axes[p][2], axes[p][3]
            if n == 0:
                own_loads[p][2].wait()
                arrived(pair[p][2], size(par.at[p, 2]))
                for side in range(2):
                    arrived(from_side[p][side], size(rcv2.at[p, side]) // 2)
            for h in range(2):
                arrived(relay[p][h][n], V * widths[n] * 4 / 1024)
                cols = pl.ds(col(half_subs[p][n][h] * SUB + starts[n], SUB // 2), widths[n])

                @pl.loop(0, V // TILE)
                def _(t):
                    rows = pl.ds(pl.multiple_of(t * TILE, TILE), TILE)
                    near = own[p, 2, rows, cols].astype(F32) + par[p, 2, rows, cols].astype(F32)
                    s_buf[p, rows, cols] = near + rcv2[p, 0, rows, cols] + rcv2[p, 1, rows, cols]

            opp2 = roles2[p][3]
            if n == 0:
                targets = ((opp2, 0), (i2 + 1 - 2 * lax.rem(i2, 2), 1))
            else:
                targets = ((opp2 + 1 - 2 * lax.rem(opp2, 2), 2),)
            for target, slot in targets:
                cols = pl.ds(col(target * SUB + starts[n], SUB // 2), widths[n])
                send(s_buf.at[p, :, cols], p2f.at[p, slot, :, starts[n]:starts[n] + widths[n]], second[p][n],
                     **{axis2: target})
        if n < 2:
            pass_state(2 + n)

    third = [[group() for _ in range(2)] for _ in range(2)]
    for q in range(2):
        for p in range(2):
            i2 = axes[p][3]
            if q == 0:
                arrived(second[p][0], 2 * V * SUB * 4 / 1024)
            arrived(second[p][1 + q], V * SUB * 2 / 1024)
            cols = pl.ds(col(i2 * SUB + q * (SUB // 2), SUB // 2), SUB // 2)
            cq = pl.ds(q * (SUB // 2), SUB // 2)

            @pl.loop(0, V // TILE)
            def _(t):
                rows = pl.ds(pl.multiple_of(t * TILE, TILE), TILE)
                t_buf[p, q, rows, :] = s_buf[p, rows, cols] + p2f[p, 0, rows, cq] + (
                    p2f[p, 1, rows, cq] + p2f[p, 2, rows, cq])

            for d in (4, 3, 5, 2, 6, 1, 7):
                zd = mod(z + d, 8)
                rows = pl.ds(pl.multiple_of(zd * TILE, TILE), TILE)
                send(t_buf.at[p, q, rows, :], z_buf.at[p, q, d - 1], third[p][q], z=zd)

    square = jnp.zeros((8, 128), F32)
    for q in range(2):
        for p in range(2):
            arrived(third[p][q], size(z_buf.at[p, q]))
            g = t_buf[p, q, my_rows, :]
            for d in range(7):
                g = g + z_buf[p, q, d]
            cq = slice(q * (SUB // 2), (q + 1) * (SUB // 2))
            g_buf[p, :, cq] = g
            g_col[p, my_rows, cq] = g
            sq = g * g
            square = square + sq[0:8] + sq[8:16]
    norm_zc, norm_xy, q1, q2, column_g = (group() for _ in range(5))
    slot = 2 * z + c
    nzc[slot] = jnp.sum(square, axis=0, keepdims=True)
    for dev in zc_peers:
        send(nzc.at[slot], nzc.at[slot], norm_zc, **dev)
    for d in (4, 3, 5, 2, 6, 1, 7):
        send(g_buf, g_col.at[:, my_rows, :], column_g, z=mod(z + d, 8))

    for p in range(2):
        for k in range(8):
            q_s[k, p] = g_buf[p, 2 * k:2 * k + 2, :]
    for k, dev in xc_peers:
        send(q_s.at[k], q_r.at[own_k], q1, **dev)
    q_r[own_k] = q_s[own_k]

    arrived_words(norm_zc, nzc)
    slot = 4 * x + y
    nxy[slot] = functools.reduce(lambda a, b: a + b, [nzc[k] for k in range(16)])
    for dev in xy_peers:
        send(nxy.at[slot], nxy.at[slot], norm_xy, **dev)

    arrived(q1, 7 * 4)
    for d in (2, 1, 3):
        send(q_r, g_full.at[y], q2, y=mod(y + d, 4))
    g_full[y] = q_r[...]

    arrived_words(norm_xy, nxy)
    total = functools.reduce(lambda a, b: a + b, [nxy[k] for k in range(16)])
    total = jnp.sum(total, axis=1, keepdims=True)
    clip = 1.0 / jnp.maximum(jnp.sqrt(total), 1.0)

    block_of = lambda p, i, j: pl.ds(col(p * HALF + i * WIDE + j * SUB, SUB), SUB)
    to_pair = group()
    rows_half = (pl.ds(0, V // 2), pl.ds(V // 2, V // 2))
    block_kib = V * SUB * 2 // 1024

    def finished(p, i, j):
        ref = o_w.at[c, :, block_of(p, i, j)]
        send(ref, ref, to_pair, c=other)

    def spread(p, i, j, axis, targets):
        ref = o_w.at[c, :, block_of(p, i, j)]
        ks = [group() for _ in targets]
        for k, target in zip(ks, targets):
            send(ref, ref, k, **{axis: target})
        return ks

    def first_targets(p, s):
        return roles[p][:2] + ((roles[p][3],) if s in DIRECT else ())

    def forward(p, i, j, axis, target, h, k):
        ref = o_w.at[c, rows_half[h], block_of(p, i, j)]
        send(ref, ref, k, **{axis: target})

    arrived(column_state[3], 96)
    arrived(column_g, 7 * 32)
    along2, along1 = [None] * 2, [[None] * 4 for _ in range(2)]
    for p in range(2):
        a1, i1, a2, i2 = axes[p]
        cols = block_of(p, i1, i2)

        @pl.loop(0, V // TILE)
        def _(t):
            rows = pl.ds(pl.multiple_of(t * TILE, TILE), TILE)
            _, _, fresh = adam(st[0, p, rows], st[1, p, rows], clip * g_col[p, rows], st[2, p, rows])
            o_w[c, rows, cols] = fresh.astype(BF16)

        right2, left2, _, opp2 = roles2[p]
        along2[p] = spread(p, i1, i2, a2, (right2, left2, opp2))
    for p in range(2):
        a1, i1, a2, i2 = axes[p]
        along1[p][0] = spread(p, i1, i2, a1, first_targets(p, 0))
        finished(p, i1, i2)

    for n, s in ((1, 1), (0, 2), (2, 3)):
        for p in range(2):
            a1, i1, a2, i2 = axes[p]
            right2, left2, _, opp2 = roles2[p]
            origin = (left2, right2, opp2)[n]
            arrived(along2[p][n], block_kib)
            along1[p][s] = spread(p, i1, origin, a1, first_targets(p, s))
            finished(p, i1, origin)

    fwd1 = [[None if s in DIRECT else group() for s in range(4)] for _ in range(2)]

    def column(p, s):
        right2, left2, _, opp2 = roles2[p]
        return (axes[p][3], right2, left2, opp2)[s]

    def pass_on(p, s):
        right1, left1, _, _ = roles[p]
        for side, origin in ((0, left1), (1, right1)):
            arrived(along1[p][s][side], block_kib)
            if s not in DIRECT:
                forward(p, origin, column(p, s), axes[p][0], roles[p][side], side, fwd1[p][s])
            finished(p, origin, column(p, s))

    arrived(q2, 3 * 32)
    lane4 = lax.broadcasted_iota(jnp.int32, (2, 4), 1)
    for m in range(2):
        tops_m = jnp.zeros((2, 4), F32)
        tops_v = jnp.zeros((2, 4), F32)
        for b in range(4):
            cs = slice(b * BLOCK, (b + 1) * BLOCK)
            pieces = []
            for s in range(8):
                if b < 2:
                    px, py, p = 2 * b + s // 4, s % 4, 0
                else:
                    py, px, p = 2 * (b - 2) + s // 4, s % 4, 1
                pieces.append(g_full[py, 2 * px + m, p])
            g = jnp.concatenate(pieces, axis=1)
            moment = l_mc[m, :, cs].astype(F32) * l_ms[m, :, b:b + 1]
            second_ = l_vc[m, :, cs].astype(F32) * l_vs[m, :, b:b + 1]
            m2, v2, fresh = adam(moment, second_, clip * g, l_master[m, :, cs])
            m_top = jnp.max(jnp.abs(m2), axis=1, keepdims=True) + 1e-20
            v_top = jnp.max(jnp.abs(v2), axis=1, keepdims=True) + 1e-20
            o_master[m, :, cs] = fresh
            o_mc[m, :, cs] = (m2 / m_top).astype(BF16)
            o_vc[m, :, cs] = (v2 / v_top).astype(BF16)
            tops_m = jnp.where(lane4 == b, m_top, tops_m)
            tops_v = jnp.where(lane4 == b, v_top, tops_v)
        o_ms[m] = tops_m
        o_vs[m] = tops_v
    for s in range(4):
        for p in range(2):
            pass_on(p, s)
    for s in range(4):
        for p in range(2):
            arrived(along1[p][s][2] if s in DIRECT else fwd1[p][s], block_kib)
            finished(p, roles[p][3], column(p, s))
    arrived(to_pair, size(o_w.at[0]))
    all_sent()
    assert groups[0] <= SEMS and groups[1] <= LOCAL_SEMS, (groups, sent)


def write_out(*refs):
    sems = refs[12]
    copies = [pltpu.make_async_copy(refs[k], refs[k + 6], sems.at[k]) for k in (5, 0, 1, 2, 3, 4)]
    for copy in copies:
        copy.start()
    for copy in copies:
        copy.wait()


def body(partials, master, m_codes, v_codes, m_scales, v_scales):
    any_spec = pl.BlockSpec(memory_space=pl.ANY)
    vmem = pltpu.VMEM
    small = [pltpu.with_memory_space_constraint(a, pltpu.HBM) for a in (master, m_codes, v_codes, m_scales, v_scales)]
    results = pl.pallas_call(
        kernel,
        out_shape=(
            jax.ShapeDtypeStruct(master.shape, F32),
            jax.ShapeDtypeStruct(master.shape, BF16),
            jax.ShapeDtypeStruct(master.shape, BF16),
            jax.ShapeDtypeStruct(m_scales.shape, F32),
            jax.ShapeDtypeStruct(m_scales.shape, F32),
            jax.ShapeDtypeStruct((2, V, D), BF16),
        ),
        in_specs=[pl.BlockSpec(memory_space=pltpu.HBM)] * 6,
        out_specs=(pl.BlockSpec(memory_space=pltpu.VMEM),) * 6,
        scratch_shapes=[
            vmem((2, 3, V, WIDE), BF16),
            vmem((2, 3, V, WIDE), BF16),
            vmem((2, 2, 2, V, WIDE // 2), BF16),
            vmem((2, 2, V, WIDE), F32),
            vmem((2, 2, V, WIDE), F32),
            vmem((2, V, WIDE), F32),
            vmem((2, 3, V, SUB), F32),
            vmem((2, 2, V, SUB // 2), F32),
            vmem((2, 2, 7, TILE, SUB // 2), F32),
            vmem((2, TILE, SUB), F32),
            vmem((16, 1, 128), F32),
            vmem((16, 1, 128), F32),
            vmem((8, 2, 2, SUB), F32),
            vmem((8, 2, 2, SUB), BF16),
            vmem((8, 2, 2, SUB), BF16),
            vmem((8, 4, 128), F32),
            vmem((2, 4, 128), F32),
            vmem((3, 2, TILE, SUB), F32),
            vmem((3, 2, V, SUB), F32),
            vmem((2, V, SUB), F32),
            vmem((8, 2, 2, SUB), F32),
            vmem((8, 2, 2, SUB), F32),
            vmem((4, 8, 2, 2, SUB), F32),
            vmem((2, 2, D), F32),
            vmem((2, 2, D), BF16),
            vmem((2, 2, D), BF16),
            vmem((2, 2, 4), F32),
            vmem((2, 2, 4), F32),
            vmem((2 * LIMIT_KIB, 1, 128), F32),
            pltpu.SemaphoreType.DMA((1,)),
            pltpu.SemaphoreType.DMA((SEMS,)),
            pltpu.SemaphoreType.DMA((LOCAL_SEMS,)),
        ],
        compiler_params=pltpu.CompilerParams(
            collective_id=0, has_side_effects=True, vmem_limit_bytes=48 * 1024 * 1024
        ),
        name="step",
    )(partials, *small)
    return pl.pallas_call(
        write_out,
        out_shape=tuple(jax.ShapeDtypeStruct(a.shape, a.dtype) for a in results),
        in_specs=[any_spec] * 6,
        out_specs=(any_spec,) * 6,
        scratch_shapes=[pltpu.SemaphoreType.DMA((6,))],
        compiler_params=pltpu.CompilerParams(vmem_limit_bytes=1024 * 1024),
        name="write_out",
    )(*results)


def solution(mesh):
    finer = Mesh(mesh.devices.reshape(NZ, NX, NC, NY), ("z", "x", "c", "y"))
    rows = P(None, ("z", "x", "c"), None)
    return jax.shard_map(
        body,
        mesh=finer,
        in_specs=(P("y", ("z", "x", "c"), None, None, None),) + (rows,) * 5,
        out_specs=(rows,) * 5 + (P(),),
        check_vma=False,
    )
```

```python
import functools
import math

import jax
import jax.numpy as jnp
from jax import lax
from jax.experimental import pallas as pl
from jax.experimental.pallas import tpu as pltpu
from jax.sharding import Mesh
from jax.sharding import PartitionSpec as P

BLOCK = 2048
STEP = 10
MESH = pl.DeviceIdType.MESH
F32 = jnp.float32
BF16 = jnp.bfloat16

V = 128
D = 8192
HALF = 4096
WIDE = 1024
SUB = 256
NX, NY, NZ, NC = 4, 4, 8, 2
TILE = 16
SEMS = 73
LOCAL_SEMS = 17
DIRECT = (3,)
LIMIT_KIB = 12 * 1024


def mod(a, n):
    return lax.rem(a + n, n)


def col(value, step):
    return pl.multiple_of(value, step)


def adam(moment, second, scaled, master):
    m2 = 0.9 * moment + 0.1 * scaled
    v2 = 0.95 * second + 0.05 * scaled * scaled
    root = jnp.sqrt(v2 * (1.0 / (1.0 - 0.95**STEP))) + 1e-08
    return m2, v2, master - m2 * (0.01 / (1.0 - 0.9**STEP)) / root


def kernel(
    part_in, master_in, mc_in, vc_in, ms_in, vs_in,
    o_master, o_mc, o_vc, o_ms, o_vs, o_w,
    own, par, rcv1, snd, rcv2, s_buf, p2f, t_buf, z_buf, g_buf,
    nzc, nxy,
    e_master, e_mc, e_vc, e_s, sc_stage, tile, st, g_col,
    q_s, q_r, g_full,
    l_master, l_mc, l_vc, l_ms, l_vs, bytes_ref,
    ssem, rsem, lsem,
):
    x, y, z, c = (lax.axis_index(a) for a in ("x", "y", "z", "c"))
    other = 1 - c
    groups, sent = [0, 0], [0]

    def size(ref):
        return math.prod(ref.shape) * ref.dtype.itemsize / 1024

    def group():
        groups[0] += 1
        return groups[0] - 1

    def send(src, dst, k, **dev):
        sent[0] += size(src)
        pltpu.make_async_remote_copy(
            src_ref=src, dst_ref=dst, send_sem=ssem.at[0], recv_sem=rsem.at[k],
            device_id=dev, device_id_type=MESH,
        ).start()

    def arrived(k, kib):
        ref = bytes_ref.at[pl.ds(0, int(2 * kib))]
        pltpu.make_async_copy(ref, ref, rsem.at[k]).wait()

    def arrived_words(k, slots):
        arrived(k, 15 * size(slots.at[0]))

    def all_sent():
        assert sent[0] <= LIMIT_KIB
        ref = bytes_ref.at[pl.ds(0, int(2 * sent[0]))]
        pltpu.make_async_copy(ref, ref, ssem.at[0]).wait()


    def local(src, dst):
        groups[1] += 1
        copy = pltpu.make_async_copy(src, dst, lsem.at[groups[1] - 1])
        copy.start()
        return copy


    axes = (("x", x, "y", y), ("y", y, "x", x))
    roles = [tuple(mod(i + d, 4) for d in (1, -1, 0, 2)) for _, i, _, _ in axes]
    roles2 = [tuple(mod(j + d, 4) for d in (1, -1, 0, 2)) for _, _, _, j in axes]
    own_k = 2 * x + c

    own_loads = [[None] * 3 for _ in range(2)]
    for role in range(3):
        for p in range(2):
            cols = pl.ds(col(p * HALF + roles[p][role] * WIDE, WIDE), WIDE)
            own_loads[p][role] = local(part_in.at[0, 0, c, :, cols], own.at[p, role])
    state_loads = [
        local(a, b)
        for a, b in (
            (ms_in, l_ms), (vs_in, l_vs), (master_in, l_master), (mc_in, l_mc), (vc_in, l_vc),
        )
    ]

    barrier = pltpu.get_barrier_semaphore()
    xc_peers, xy_peers, zc_peers = [], [], []
    for d in range(1, 8):
        k = mod(own_k + d, 8)
        xc_peers.append((k, {"x": k // 2, "c": lax.rem(k, 2)}))
    for d in (10, 9, 11, 6, 14, 2, 8, 5, 7, 13, 15, 1, 3, 4, 12):
        xy_peers.append({"x": mod(x + d // 4, 4), "y": mod(y + d % 4, 4)})
    for d in (8, 9, 6, 7, 10, 11, 4, 5, 12, 13, 2, 3, 14, 15, 1):
        zc_peers.append({"z": mod(z + d // 2, 8), "c": lax.rem(c + d % 2, 2)})
    greeted = list(xy_peers) + list(zc_peers)
    greeted += [{"x": mod(x + d, 4), "c": other} for d in (1, 2, 3)]
    greeted += [{"y": mod(y + d, 4), "c": other} for d in (1, 3)]
    for dev in greeted:
        pl.semaphore_signal(barrier, inc=1, device_id=dev, device_id_type=MESH)
    pl.semaphore_wait(barrier, len(greeted))

    raw = [[group() for _ in range(2)] for _ in range(2)]
    for q in range(2):
        m = lax.rem(c + q, 2)
        for p in range(2):
            axis = axes[p][0]
            for h in range(2):
                cols = pl.ds(col(p * HALF + roles[p][3] * WIDE + h * (WIDE // 2), WIDE // 2), WIDE // 2)
                send(part_in.at[0, 0, m, :, cols], rcv1.at[p, h, q], raw[p][h], **{axis: roles[p][h], "c": m})
    pair = [[group() for _ in range(3)] for _ in range(2)]
    for role in range(3):
        for p in range(2):
            cols = pl.ds(col(p * HALF + roles[p][role] * WIDE, WIDE), WIDE)
            send(part_in.at[0, 0, other, :, cols], par.at[p, role], pair[p][role], c=other)

    state = group()
    tile_cols = [
        lambda kx: col(kx * WIDE + y * SUB, SUB),
        lambda kx: col(HALF + y * WIDE + kx * SUB, SUB),
    ]
    own_state = []
    for src, dst in ((master_in, e_master), (mc_in, e_mc), (vc_in, e_vc)):
        for p in range(2):
            own_state.append(local(src.at[c, :, pl.ds(tile_cols[p](x), SUB)], dst.at[own_k, p]))
            for k, dev in xc_peers:
                send(src.at[dev["c"], :, pl.ds(tile_cols[p](dev["x"]), SUB)], dst.at[own_k, p], state, **dev)
    for load in state_loads:
        load.wait()
    sc_stage[...] = jnp.zeros_like(sc_stage)
    for m in range(2):
        sc_stage[m, 0:2, 0:4] = l_ms[m]
        sc_stage[m, 2:4, 0:4] = l_vs[m]
    e_s[own_k] = sc_stage[c]
    for k, dev in xc_peers:
        send(sc_stage.at[dev["c"]], e_s.at[own_k], state, **dev)

    from_side = [group() for _ in range(2)]
    for p in range(2):
        axis = axes[p][0]
        for side in range(2):
            own_loads[p][side].wait()
            arrived(pair[p][side], size(par.at[p, side]))
            lo = (1 - side) * (WIDE // 2)

            @pl.loop(0, V // TILE)
            def _(t):
                rows = pl.ds(pl.multiple_of(t * TILE, TILE), TILE)
                cc = pl.ds(lo, WIDE // 2)
                snd[p, side, rows, cc] = own[p, side, rows, cc].astype(F32) + par[p, side, rows, cc].astype(F32)

            cc = pl.ds(lo, WIDE // 2)
            send(snd.at[p, side, :, cc], rcv2.at[p, side, :, cc], from_side[p], **{axis: roles[p][side]})

    for copy in own_state:
        copy.wait()
    arrived(state, 7 * 10)
    blocks = (x // 2, 2 + y // 2)
    for k in range(8):
        e = e_s[k]
        lane = lax.broadcasted_iota(jnp.int32, e.shape, 1)
        for p in range(2):
            scale = jnp.sum(jnp.where(lane == blocks[p], e, 0.0), axis=1, keepdims=True)
            rows = pl.ds(2 * k, 2)
            tile[0, p, rows, :] = e_mc[k, p].astype(F32) * scale[0:2]
            tile[1, p, rows, :] = e_vc[k, p].astype(F32) * scale[2:4]
            tile[2, p, rows, :] = e_master[k, p]
    my_rows = pl.ds(pl.multiple_of(z * TILE, TILE), TILE)
    z_next, z_last = {"z": mod(z + 1, 8)}, {"z": mod(z - 1, 8)}
    z_rows = lambda d: pl.ds(pl.multiple_of(mod(z + d, 8) * TILE, TILE), TILE)
    column_state = [group() for _ in range(4)]
    send(tile, st.at[:, :, my_rows, :], column_state[0], **z_next)
    send(tile, st.at[:, :, my_rows, :], column_state[0], **z_last)

    def pass_state(n):
        arrived(column_state[n - 1], 2 * 96)
        for d, dev, p in ((-n, z_next, 0), (n, z_last, 1)):
            ref = st.at[:, :, z_rows(d), :] if n < 3 else st.at[:, p, z_rows(d), :]
            send(ref, ref, column_state[n], **dev)

    for n in range(3):
        for p in range(2):
            st[n, p, my_rows, :] = tile[n, p]

    half_subs = []
    for p in range(2):
        i2 = axes[p][3]
        half_subs.append([
            tuple(2 * h + lax.rem(i2 + i2 // 2 + h + 1 - min(n, 1), 2) for h in range(2)) for n in range(3)
        ])
    starts, widths = (0, 0, SUB // 2), (SUB, SUB // 2, SUB // 2)
    relay = [[group() for _ in range(3)] for _ in range(2)]
    for n in range(3):
        for p in range(2):
            axis = axes[p][0]
            for side in range(2):
                sub = half_subs[p][n][side]
                if n == 0:
                    arrived(raw[p][side], size(rcv1.at[p, side]))
                cc = pl.ds(col(sub * SUB + starts[n], SUB // 2), widths[n])
                cr = pl.ds(col((sub - 2 * side) * SUB + starts[n], SUB // 2), widths[n])

                @pl.loop(0, V // TILE)
                def _(t):
                    rows = pl.ds(pl.multiple_of(t * TILE, TILE), TILE)
                    near = own[p, side, rows, cc].astype(F32) + par[p, side, rows, cc].astype(F32)
                    far = rcv1[p, side, 0, rows, cr].astype(F32) + rcv1[p, side, 1, rows, cr].astype(F32)
                    snd[p, side, rows, cc] = near + far

                send(snd.at[p, side, :, cc], rcv2.at[p, side, :, cc], relay[p][n], **{axis: roles[p][side]})
    pass_state(1)

    second = [[group() for _ in range(3)] for _ in range(2)]
    for n in range(3):
        for p in range(2):
            axis2, i2 = axes[p][2], axes[p][3]
            if n == 0:
                own_loads[p][2].wait()
                arrived(pair[p][2], size(par.at[p, 2]))
                arrived(from_side[p], size(rcv2.at[p, 0]))
            arrived(relay[p][n], 2 * V * widths[n] * 4 / 1024)
            for h in range(2):
                cols = pl.ds(col(half_subs[p][n][h] * SUB + starts[n], SUB // 2), widths[n])

                @pl.loop(0, V // TILE)
                def _(t):
                    rows = pl.ds(pl.multiple_of(t * TILE, TILE), TILE)
                    near = own[p, 2, rows, cols].astype(F32) + par[p, 2, rows, cols].astype(F32)
                    s_buf[p, rows, cols] = near + rcv2[p, 0, rows, cols] + rcv2[p, 1, rows, cols]

            opp2 = roles2[p][3]
            if n == 0:
                targets = ((opp2, 0), (i2 + 1 - 2 * lax.rem(i2, 2), 1))
            else:
                targets = ((opp2 + 1 - 2 * lax.rem(opp2, 2), 2),)
            for target, slot in targets:
                cols = pl.ds(col(target * SUB + starts[n], SUB // 2), widths[n])
                send(s_buf.at[p, :, cols], p2f.at[p, slot, :, starts[n]:starts[n] + widths[n]], second[p][n],
                     **{axis2: target})
        if n < 2:
            pass_state(2 + n)

    third = [[group() for _ in range(2)] for _ in range(2)]
    for q in range(2):
        for p in range(2):
            i2 = axes[p][3]
            if q == 0:
                arrived(second[p][0], 2 * V * SUB * 4 / 1024)
            arrived(second[p][1 + q], V * SUB * 2 / 1024)
            cols = pl.ds(col(i2 * SUB + q * (SUB // 2), SUB // 2), SUB // 2)
            cq = pl.ds(q * (SUB // 2), SUB // 2)

            @pl.loop(0, V // TILE)
            def _(t):
                rows = pl.ds(pl.multiple_of(t * TILE, TILE), TILE)
                t_buf[p, q, rows, :] = s_buf[p, rows, cols] + p2f[p, 0, rows, cq] + (
                    p2f[p, 1, rows, cq] + p2f[p, 2, rows, cq])

            for d in (4, 3, 5, 2, 6, 1, 7):
                zd = mod(z + d, 8)
                rows = pl.ds(pl.multiple_of(zd * TILE, TILE), TILE)
                send(t_buf.at[p, q, rows, :], z_buf.at[p, q, d - 1], third[p][q], z=zd)

    square = jnp.zeros((8, 128), F32)
    for q in range(2):
        for p in range(2):
            arrived(third[p][q], size(z_buf.at[p, q]))
            g = t_buf[p, q, my_rows, :]
            for d in range(7):
                g = g + z_buf[p, q, d]
            cq = slice(q * (SUB // 2), (q + 1) * (SUB // 2))
            g_buf[p, :, cq] = g
            g_col[p, my_rows, cq] = g
            sq = g * g
            square = square + sq[0:8] + sq[8:16]
    norm_zc, norm_xy, q1, q2, column_g = (group() for _ in range(5))
    slot = 2 * z + c
    nzc[slot] = jnp.sum(square, axis=0, keepdims=True)
    for dev in zc_peers:
        send(nzc.at[slot], nzc.at[slot], norm_zc, **dev)
    for d in (4, 3, 5, 2, 6, 1, 7):
        send(g_buf, g_col.at[:, my_rows, :], column_g, z=mod(z + d, 8))

    for p in range(2):
        for k in range(8):
            q_s[k, p] = g_buf[p, 2 * k:2 * k + 2, :]
    for k, dev in xc_peers:
        send(q_s.at[k], q_r.at[own_k], q1, **dev)
    q_r[own_k] = q_s[own_k]

    arrived_words(norm_zc, nzc)
    slot = 4 * x + y
    nxy[slot] = functools.reduce(lambda a, b: a + b, [nzc[k] for k in range(16)])
    for dev in xy_peers:
        send(nxy.at[slot], nxy.at[slot], norm_xy, **dev)

    arrived(q1, 7 * 4)
    for d in (2, 1, 3):
        send(q_r, g_full.at[y], q2, y=mod(y + d, 4))
    g_full[y] = q_r[...]

    arrived_words(norm_xy, nxy)
    total = functools.reduce(lambda a, b: a + b, [nxy[k] for k in range(16)])
    total = jnp.sum(total, axis=1, keepdims=True)
    clip = 1.0 / jnp.maximum(jnp.sqrt(total), 1.0)

    block_of = lambda p, i, j: pl.ds(col(p * HALF + i * WIDE + j * SUB, SUB), SUB)
    to_pair = group()
    rows_half = (pl.ds(0, V // 2), pl.ds(V // 2, V // 2))
    block_kib = V * SUB * 2 // 1024

    def finished(p, i, j):
        ref = o_w.at[c, :, block_of(p, i, j)]
        send(ref, ref, to_pair, c=other)

    def spread(p, i, j, axis, targets):
        ref = o_w.at[c, :, block_of(p, i, j)]
        ks = [group() for _ in targets]
        for k, target in zip(ks, targets):
            send(ref, ref, k, **{axis: target})
        return ks

    def first_targets(p, s):
        return roles[p][:2] + ((roles[p][3],) if s in DIRECT else ())

    def forward(p, i, j, axis, target, h, k):
        ref = o_w.at[c, rows_half[h], block_of(p, i, j)]
        send(ref, ref, k, **{axis: target})

    arrived(column_state[3], 96)
    arrived(column_g, 7 * 32)
    along2, along1 = [None] * 2, [[None] * 4 for _ in range(2)]
    for p in range(2):
        a1, i1, a2, i2 = axes[p]
        cols = block_of(p, i1, i2)

        @pl.loop(0, V // TILE)
        def _(t):
            rows = pl.ds(pl.multiple_of(t * TILE, TILE), TILE)
            _, _, fresh = adam(st[0, p, rows], st[1, p, rows], clip * g_col[p, rows], st[2, p, rows])
            o_w[c, rows, cols] = fresh.astype(BF16)

        right2, left2, _, opp2 = roles2[p]
        along2[p] = spread(p, i1, i2, a2, (right2, left2, opp2))
    for p in range(2):
        a1, i1, a2, i2 = axes[p]
        along1[p][0] = spread(p, i1, i2, a1, first_targets(p, 0))
        finished(p, i1, i2)

    for n, s in ((1, 1), (0, 2), (2, 3)):
        for p in range(2):
            a1, i1, a2, i2 = axes[p]
            right2, left2, _, opp2 = roles2[p]
            origin = (left2, right2, opp2)[n]
            arrived(along2[p][n], block_kib)
            along1[p][s] = spread(p, i1, origin, a1, first_targets(p, s))
            finished(p, i1, origin)

    fwd1 = [[None if s in DIRECT else group() for s in range(4)] for _ in range(2)]

    def column(p, s):
        right2, left2, _, opp2 = roles2[p]
        return (axes[p][3], right2, left2, opp2)[s]

    def pass_on(p, s):
        right1, left1, _, _ = roles[p]
        for side, origin in ((0, left1), (1, right1)):
            arrived(along1[p][s][side], block_kib)
            if s not in DIRECT:
                forward(p, origin, column(p, s), axes[p][0], roles[p][side], side, fwd1[p][s])
            finished(p, origin, column(p, s))

    arrived(q2, 3 * 32)
    lane4 = lax.broadcasted_iota(jnp.int32, (2, 4), 1)
    for m in range(2):
        tops_m = jnp.zeros((2, 4), F32)
        tops_v = jnp.zeros((2, 4), F32)
        for b in range(4):
            cs = slice(b * BLOCK, (b + 1) * BLOCK)
            pieces = []
            for s in range(8):
                if b < 2:
                    px, py, p = 2 * b + s // 4, s % 4, 0
                else:
                    py, px, p = 2 * (b - 2) + s // 4, s % 4, 1
                pieces.append(g_full[py, 2 * px + m, p])
            g = jnp.concatenate(pieces, axis=1)
            moment = l_mc[m, :, cs].astype(F32) * l_ms[m, :, b:b + 1]
            second_ = l_vc[m, :, cs].astype(F32) * l_vs[m, :, b:b + 1]
            m2, v2, fresh = adam(moment, second_, clip * g, l_master[m, :, cs])
            m_top = jnp.max(jnp.abs(m2), axis=1, keepdims=True) + 1e-20
            v_top = jnp.max(jnp.abs(v2), axis=1, keepdims=True) + 1e-20
            o_master[m, :, cs] = fresh
            o_mc[m, :, cs] = (m2 / m_top).astype(BF16)
            o_vc[m, :, cs] = (v2 / v_top).astype(BF16)
            tops_m = jnp.where(lane4 == b, m_top, tops_m)
            tops_v = jnp.where(lane4 == b, v_top, tops_v)
        o_ms[m] = tops_m
        o_vs[m] = tops_v
    for s in range(4):
        for p in range(2):
            pass_on(p, s)
    for s in range(4):
        for p in range(2):
            arrived(along1[p][s][2] if s in DIRECT else fwd1[p][s], block_kib)
            finished(p, roles[p][3], column(p, s))
    arrived(to_pair, size(o_w.at[0]))
    all_sent()
    assert groups[0] <= SEMS and groups[1] <= LOCAL_SEMS, (groups, sent)


def write_out(*refs):
    sems = refs[12]
    copies = [pltpu.make_async_copy(refs[k], refs[k + 6], sems.at[k]) for k in (5, 0, 1, 2, 3, 4)]
    for copy in copies:
        copy.start()
    for copy in copies:
        copy.wait()


def body(partials, master, m_codes, v_codes, m_scales, v_scales):
    any_spec = pl.BlockSpec(memory_space=pl.ANY)
    vmem = pltpu.VMEM
    small = [pltpu.with_memory_space_constraint(a, pltpu.HBM) for a in (master, m_codes, v_codes, m_scales, v_scales)]
    results = pl.pallas_call(
        kernel,
        out_shape=(
            jax.ShapeDtypeStruct(master.shape, F32),
            jax.ShapeDtypeStruct(master.shape, BF16),
            jax.ShapeDtypeStruct(master.shape, BF16),
            jax.ShapeDtypeStruct(m_scales.shape, F32),
            jax.ShapeDtypeStruct(m_scales.shape, F32),
            jax.ShapeDtypeStruct((2, V, D), BF16),
        ),
        in_specs=[pl.BlockSpec(memory_space=pltpu.HBM)] * 6,
        out_specs=(pl.BlockSpec(memory_space=pltpu.VMEM),) * 6,
        scratch_shapes=[
            vmem((2, 3, V, WIDE), BF16),
            vmem((2, 3, V, WIDE), BF16),
            vmem((2, 2, 2, V, WIDE // 2), BF16),
            vmem((2, 2, V, WIDE), F32),
            vmem((2, 2, V, WIDE), F32),
            vmem((2, V, WIDE), F32),
            vmem((2, 3, V, SUB), F32),
            vmem((2, 2, V, SUB // 2), F32),
            vmem((2, 2, 7, TILE, SUB // 2), F32),
            vmem((2, TILE, SUB), F32),
            vmem((16, 1, 128), F32),
            vmem((16, 1, 128), F32),
            vmem((8, 2, 2, SUB), F32),
            vmem((8, 2, 2, SUB), BF16),
            vmem((8, 2, 2, SUB), BF16),
            vmem((8, 4, 128), F32),
            vmem((2, 4, 128), F32),
            vmem((3, 2, TILE, SUB), F32),
            vmem((3, 2, V, SUB), F32),
            vmem((2, V, SUB), F32),
            vmem((8, 2, 2, SUB), F32),
            vmem((8, 2, 2, SUB), F32),
            vmem((4, 8, 2, 2, SUB), F32),
            vmem((2, 2, D), F32),
            vmem((2, 2, D), BF16),
            vmem((2, 2, D), BF16),
            vmem((2, 2, 4), F32),
            vmem((2, 2, 4), F32),
            vmem((2 * LIMIT_KIB, 1, 128), F32),
            pltpu.SemaphoreType.DMA((1,)),
            pltpu.SemaphoreType.DMA((SEMS,)),
            pltpu.SemaphoreType.DMA((LOCAL_SEMS,)),
        ],
        compiler_params=pltpu.CompilerParams(
            collective_id=0, has_side_effects=True, vmem_limit_bytes=48 * 1024 * 1024
        ),
        name="step",
    )(partials, *small)
    return pl.pallas_call(
        write_out,
        out_shape=tuple(jax.ShapeDtypeStruct(a.shape, a.dtype) for a in results),
        in_specs=[any_spec] * 6,
        out_specs=(any_spec,) * 6,
        scratch_shapes=[pltpu.SemaphoreType.DMA((6,))],
        compiler_params=pltpu.CompilerParams(vmem_limit_bytes=1024 * 1024),
        name="write_out",
    )(*results)


def solution(mesh):
    finer = Mesh(mesh.devices.reshape(NZ, NX, NC, NY), ("z", "x", "c", "y"))
    rows = P(None, ("z", "x", "c"), None)
    return jax.shard_map(
        body,
        mesh=finer,
        in_specs=(P("y", ("z", "x", "c"), None, None, None),) + (rows,) * 5,
        out_specs=(rows,) * 5 + (P(),),
        check_vma=False,
    )
```
